256 devices in a mesh: row: 16 (over x, y), col: 16 (over z, core).
Axes of the slice: x: 4, y: 4, z: 8, core: 2. Of those that a mesh axis runs over, the one named last changes fastest.
Arguments:
- loads: float32 [16, 16, 1024, 8], P('row', 'col'), may hold values from -6 to 6
- schur: float32 [16, 16, 1024, 1024], P('row', 'col'), may hold values from -0.5 to 4.5, as said below
- factor: float32 [16, 16, 1024, 1024], P('row', 'col'), may hold values from -0.5 to 0.6, as said below
- coarse_inverse: float32 [12288, 12288], P(('row', 'col')), may hold values from -0.5 to 1.5, as said below
- elements: int32 [16, 16], P('row', 'col'), may hold values from 4096 to 16383
- west_map: int32 [16, 16, 256], P('row', 'col'), may hold values from 0 to 255, each once within a row
- south_map: int32 [16, 16, 256], P('row', 'col'), may hold values from 0 to 255, each once within a row
- prim_local: int32 [16, 16, 48], P('row', 'col'), may hold values from 0 to 1023
- prim_coarse: int32 [16, 16, 48], P('row', 'col'), may hold values from 0 to 12287
Outputs:
- solution: float32 [16, 16, 1024, 8], P('row', 'col')
- residual: float32 [16, 16, 1024, 8], P('row', 'col')
The draws below stay inside these ranges and needn't reach their ends.
Inputs may be any that keep to these rules, and one draw needn't show every extreme that they name: `schur`: symmetric positive definite. `factor`: symmetric positive definite. `coarse_inverse`: symmetric positive definite. `west_map`: each subdomain's row is a permutation of 0 to 255. `south_map`: each subdomain's row is a permutation of 0 to 255. `prim_local`: values may repeat. `prim_coarse`: values may repeat, within a subdomain and between subdomains.
All inputs are finite; a program needn't handle non-finite values.
Results may differ from the reference program's by a relative error of at most 0.0001.
Values sent between devices are 32-bit elements; how exact they have to be, the bound alone decides.
No kernel may reach another device: no remote copies, remote signals or barrier semaphores. Data moves between devices by JAX's collectives and lax.ppermute only.
A program may use at most 128 MiB of HBM per device.

```python
import math
import jax
import jax.numpy as jnp
from jax import lax

NI = 1024
NPRIM = 48
NRHS = 8
ITERS = 1
ELEM_BASE = 4096
FACE = 256
NCO = 12288
N_ROW = 16
N_COL = 16


def symmetric_noise(key, leading, order):
    shape = leading + (order, order)
    base = jnp.clip(jax.random.normal(key, shape, jnp.float32), -6.0, 6.0)
    return (base + jnp.swapaxes(base, -1, -2)) / math.sqrt(2.0)


def schur_diagonal(key):
    spread = jax.random.uniform(jax.random.fold_in(key, 3), (N_ROW, N_COL, NI), jnp.float32)
    return 2.0 * jnp.exp(spread * math.log(2.0))


def draw_schur(key, part):
    diagonal = schur_diagonal(key)
    noise = symmetric_noise(jax.random.fold_in(key, 7), (N_ROW, N_COL), NI)
    return diagonal[..., None] * jnp.eye(NI, dtype=jnp.float32) + 0.5 / math.sqrt(NI) * noise


def draw_factor(key, part):
    diagonal = schur_diagonal(key)
    noise = symmetric_noise(jax.random.fold_in(key, 9), (N_ROW, N_COL), NI)
    return (1.0 / diagonal)[..., None] * jnp.eye(NI, dtype=jnp.float32) + 0.04 / math.sqrt(NI) * noise


def draw_coarse_inverse(key, part):
    diagonal = 0.5 + 0.5 * jax.random.uniform(jax.random.fold_in(key, 5), (NCO,), jnp.float32)
    noise = symmetric_noise(jax.random.fold_in(key, 13), (), NCO)
    return diagonal[:, None] * jnp.eye(NCO, dtype=jnp.float32) + 0.15 / math.sqrt(NCO) * noise


def with_ends(values, rng, smallest, high):
    longest = values.shape.index(max(values.shape))
    spots = []
    for shift in (0, 1):
        where = [jax.random.randint(jax.random.fold_in(rng, axis), (), 0, length) for axis, length in enumerate(values.shape)]
        where[longest] = (where[longest] + shift) % values.shape[longest]
        spots.append(tuple(where))
    return values.at[spots[0]].set(smallest).at[spots[1]].set(high)


def steps_of(own_key, shape, pieces, low, high):
    gain, own = 1.0, jax.random.fold_in(own_key, 6)
    for position, shards_of in pieces:
        draws = jnp.exp(jax.random.uniform(jax.random.fold_in(own, position), (shards_of,), jnp.float32, low / len(pieces), high / len(pieces)))
        gain = gain * jnp.repeat(draws, shape[position] // shards_of).reshape([-1 if axis == position else 1 for axis in range(len(shape))])
    return gain


def gaussian(rng, dims, scale, limit, pieces=(), held_as=jnp.bfloat16):
    values = scale * jax.random.normal(rng, dims, jnp.float32)
    if pieces:
        values = values * steps_of(rng, dims, pieces, -0.22, 0.18)
    return jnp.clip(values, -limit, limit).astype(held_as)


def setup_inputs(seed: int = 0) -> dict:
    seeds = jax.random.split(jax.random.key(seed), 10)
    return {
        "loads": gaussian(seeds[0], (N_ROW, N_COL, NI, NRHS), 1.0, 6.0, ((0, 16), (1, 16)), jnp.float32),
        "schur": draw_schur(jax.random.fold_in(seeds[9], 71), 0),
        "factor": draw_factor(jax.random.fold_in(seeds[9], 71), 0),
        "coarse_inverse": draw_coarse_inverse(jax.random.fold_in(seeds[9], 71), 0),
        "elements": with_ends(jax.random.randint(seeds[4], (N_ROW, N_COL), ELEM_BASE, 4 * ELEM_BASE), jax.random.fold_in(seeds[4], 1), ELEM_BASE, (4 * ELEM_BASE) - 1).astype(jnp.int32),
        "west_map": jax.vmap(lambda own: jax.random.permutation(own, FACE))(jax.random.split(seeds[5], N_ROW * N_COL)).reshape((N_ROW, N_COL, FACE)).astype(jnp.int32),
        "south_map": jax.vmap(lambda own: jax.random.permutation(own, FACE))(jax.random.split(seeds[6], N_ROW * N_COL)).reshape((N_ROW, N_COL, FACE)).astype(jnp.int32),
        "prim_local": with_ends(jax.random.randint(seeds[7], (N_ROW, N_COL, NPRIM), 0, NI), jax.random.fold_in(seeds[7], 1), 0, NI - 1).astype(jnp.int32),
        "prim_coarse": with_ends(jax.random.randint(seeds[8], (N_ROW, N_COL, NPRIM), 0, NCO), jax.random.fold_in(seeds[8], 1), 0, NCO - 1).astype(jnp.int32),
    }


HIGHEST_PRECISION = lax.Precision.HIGHEST


def face_weights():
    face_ids = jnp.arange(NI) // FACE
    column_ids = jnp.arange(N_COL)
    row_ids = jnp.arange(N_ROW)
    neighbour_flags = jnp.stack([
        jnp.broadcast_to(column_ids[None, :] > 0, (N_ROW, N_COL)),
        jnp.broadcast_to(column_ids[None, :] < N_COL - 1, (N_ROW, N_COL)),
        jnp.broadcast_to(row_ids[:, None] > 0, (N_ROW, N_COL)),
        jnp.broadcast_to(row_ids[:, None] < N_ROW - 1, (N_ROW, N_COL))], axis=-1)
    return jnp.where(neighbour_flags[:, :, face_ids], 0.5, 1.0).astype(jnp.float32)[..., None]


def pick_rows(values, orders):
    return jax.vmap(jax.vmap(lambda source, places: jnp.take(source, places, axis=0)))(values, orders)


def place_rows(values, orders):
    return jax.vmap(jax.vmap(lambda source, places: jnp.zeros_like(source).at[places].set(source)))(values, orders)


def assemble(values, west_map, south_map):
    west_face = values[:, :, :FACE]
    east_face = values[:, :, FACE:2 * FACE]
    south_face = values[:, :, 2 * FACE:3 * FACE]
    north_face = values[:, :, 3 * FACE:]
    blank_column = jnp.zeros((N_ROW, 1, FACE, NRHS), jnp.float32)
    blank_row = jnp.zeros((1, N_COL, FACE, NRHS), jnp.float32)
    from_west = jnp.concatenate([blank_column, east_face[:, :-1]], axis=1)
    west_add = pick_rows(from_west, west_map)
    from_east = jnp.concatenate([place_rows(west_face, west_map)[:, 1:], blank_column], axis=1)
    from_south = jnp.concatenate([blank_row, north_face[:-1]], axis=0)
    south_add = pick_rows(from_south, south_map)
    from_north = jnp.concatenate([place_rows(south_face, south_map)[1:], blank_row], axis=0)
    return values + jnp.concatenate([west_add, from_east, south_add, from_north], axis=2)


def local_solve(operands):
    schur_block, factor_block, scaled, sweeps = operands
    first = jnp.dot(factor_block, scaled, precision=HIGHEST_PRECISION, preferred_element_type=jnp.float32)

    def sweep(turn, current):
        inner_term = jnp.dot(schur_block, current, precision=HIGHEST_PRECISION, preferred_element_type=jnp.float32)
        return current + jnp.dot(factor_block, scaled - inner_term, precision=HIGHEST_PRECISION, preferred_element_type=jnp.float32)

    return lax.fori_loop(1, sweeps, sweep, first)


def coarse_part(scaled, prim_local, prim_coarse, coarse_inverse):
    picked = pick_rows(scaled, prim_local)
    right_side = jnp.zeros((NCO, NRHS), jnp.float32).at[prim_coarse.reshape(-1)].add(picked.reshape(-1, NRHS))
    solved = jnp.dot(coarse_inverse, right_side, precision=HIGHEST_PRECISION, preferred_element_type=jnp.float32)
    spread = jnp.take(solved, prim_coarse.reshape(-1), axis=0).reshape(N_ROW, N_COL, NPRIM, NRHS)
    return jax.vmap(jax.vmap(lambda source, places: jnp.zeros((NI, NRHS), jnp.float32).at[places].add(source)))(spread, prim_local)


def reference(loads, schur, factor, coarse_inverse, elements, west_map, south_map, prim_local, prim_coarse):
    weights = face_weights()
    sweep_count = elements // ELEM_BASE

    def operator(values):
        return assemble(jnp.matmul(schur, values, precision=HIGHEST_PRECISION), west_map, south_map)

    def precondition(current):
        scaled = weights * current
        local = lax.map(local_solve, (schur.reshape(-1, NI, NI), factor.reshape(-1, NI, NI),
                                      scaled.reshape(-1, NI, NRHS), sweep_count.reshape(-1)))
        local = local.reshape(N_ROW, N_COL, NI, NRHS)
        correction = coarse_part(scaled, prim_local, prim_coarse, coarse_inverse)
        return assemble(weights * (local + correction), west_map, south_map)

    def inner(first, second):
        return jnp.sum(weights * first * second, axis=(0, 1, 2))

    right_side = assemble(loads, west_map, south_map)
    solution = jnp.zeros_like(right_side)
    residual = right_side
    precond = precondition(residual)
    direction = precond
    product_now = inner(residual, precond)
    for iteration in range(ITERS):
        image = operator(direction)
        alpha = product_now / inner(direction, image)
        solution = solution + alpha * direction
        residual = residual - alpha * image
        if iteration + 1 < ITERS:
            precond = precondition(residual)
            product_next = inner(residual, precond)
            direction = precond + (product_next / product_now) * direction
            product_now = product_next
    return solution, residual
```

```python
import jax
import jax.numpy as jnp
from jax import lax
from jax.experimental import pallas as pl
from jax.experimental.pallas import tpu as pltpu
from jax.sharding import PartitionSpec as P

ELEM_BASE = 4096
ROW, COL = "row", "col"
F32, BF16 = jnp.float32, jnp.bfloat16
VM = pl.BlockSpec(memory_space=pltpu.VMEM)
SM = pl.BlockSpec(memory_space=pltpu.SMEM)
LANES = 128
NPRIM = 48
SIDE = 16
IDX_AT = 64
RADIX = 256


def call(body, outs, specs, scratch=(), flops=0, moved=0):
    return pl.pallas_call(
        body,
        out_shape=outs,
        in_specs=specs,
        out_specs=jax.tree.map(lambda _: VM, outs),
        scratch_shapes=list(scratch),
        cost_estimate=pl.CostEstimate(flops=flops, transcendentals=0, bytes_accessed=moved),
        name=body.__name__,
    )


def shape(*dims, dtype=F32):
    return jax.ShapeDtypeStruct(dims, dtype)


def halves(x):
    high = x.astype(BF16)
    return high, (x - high.astype(F32)).astype(BF16)


def thirds(x):
    high = x.astype(BF16)
    rest = x - high.astype(F32)
    middle = rest.astype(BF16)
    low = (rest - middle.astype(F32)).astype(BF16)
    return high, middle, low


def nn(a, b):
    return lax.dot_general(a, b, (((1,), (0,)), ((), ())), preferred_element_type=F32)


def nt(a, b):
    return lax.dot_general(a, b, (((1,), (1,)), ((), ())), preferred_element_type=F32)


def one_hot(shape_, row):
    return jnp.where(lax.broadcasted_iota(jnp.int32, shape_, 0) == row, 1.0, 0.0).astype(BF16)


def selected(x, matrix, product):
    high, middle, low = thirds(x)
    return product(high, matrix) + product(middle, matrix) + product(low, matrix)


def times(x, high, low):
    x_high, x_low = halves(x)
    return nn(x_high, high) + nn(x_low, high) + nn(x_high, low)


def weight_row(row, col, unknowns):
    face = lax.broadcasted_iota(jnp.int32, (8, unknowns), 1) // (unknowns // 4)
    inner = jnp.where(face == 0, jnp.where(col > 0, 1, 0), jnp.where(col < SIDE - 1, 1, 0))
    outer = jnp.where(face == 2, jnp.where(row > 0, 1, 0), jnp.where(row < SIDE - 1, 1, 0))
    return jnp.where(jnp.where(face < 2, inner, outer) > 0, 0.5, 1.0).astype(F32)


def faces(x):
    size = x.shape[1] // 4
    return [x[:, i * size : (i + 1) * size] for i in range(4)]


def write_sends(values, orders, row, col, sends):
    west, east, south, north = faces(values)
    size = west.shape[1]
    for near, far, order, place, first, second in (
        (west, east, orders[0], col, sends[0], sends[1]),
        (south, north, orders[1], row, sends[2], sends[3]),
    ):
        back = selected(near, one_hot((size, size), order), nt)
        even = place % 2 == 0
        first[...] = jnp.where(even, far, back)
        second[...] = jnp.where(even, back, far)


def halo(got, orders, row, col):
    parts = []
    for order, place, first, second in (
        (orders[0], col, got[0], got[1]),
        (orders[1], row, got[2], got[3]),
    ):
        even = place % 2 == 0
        behind = jnp.where(even, second, first)
        ahead = jnp.where(even, first, second)
        size = behind.shape[1]
        picked = selected(behind, one_hot((size, size), order), nn)
        parts.append(jnp.where(place > 0, picked, 0.0))
        parts.append(jnp.where(place < SIDE - 1, ahead, 0.0))
    return jnp.concatenate(parts, axis=1)


def split_matrices(schur, factor, coarse, *outs):
    for k, ref in enumerate((schur, factor, coarse)):
        high, low = halves(ref[...])
        outs[2 * k][...] = high
        outs[2 * k + 1][...] = low


def first_sends(place, loads, west, south, *sends):
    write_sends(loads[...], (west[...], south[...]), place[0], place[1], sends)


def right_side(place, loads, g0, g1, g2, g3, west, south, local_at, coarse_at, b_ref, scaled_ref, slots):
    row, col = place[0], place[1]
    b = loads[...] + halo([g0[...], g1[...], g2[...], g3[...]], (west[...], south[...]), row, col)
    scaled = weight_row(row, col, b.shape[1]) * b
    b_ref[...] = b
    scaled_ref[...] = scaled
    picked = selected(scaled, one_hot((b.shape[1], LANES), local_at[...]), nn)
    lane = lax.broadcasted_iota(jnp.int32, (8, LANES), 1)
    tile = jnp.where(lane < NPRIM, picked, 0.0)
    index = jnp.broadcast_to(coarse_at[...].astype(F32), (8, LANES))
    index = pltpu.roll(index, IDX_AT, 1)
    tile = jnp.where((lane >= IDX_AT) & (lane < IDX_AT + NPRIM), index, tile)
    for i in range(SIDE):
        slots[i] = tile


def packed(tile_of, at):
    lane = lax.broadcasted_iota(jnp.int32, (8, LANES), 1)
    count = SIDE * NPRIM // LANES
    out = [jnp.zeros((8, LANES), F32) for _ in range(count)]
    for i in range(SIDE):
        start = i * NPRIM
        t, off = start // LANES, start % LANES
        moved = pltpu.roll(tile_of(i), (off - at) % LANES, 1)
        out[t] = jnp.where((lane >= off) & (lane < off + NPRIM), moved, out[t])
        if off + NPRIM > LANES:
            out[t + 1] = jnp.where(lane < off + NPRIM - LANES, moved, out[t + 1])
    return out


def pack_picked(got, coarse_at, slots):
    values = packed(lambda i: got[i], 0)
    index = packed(lambda i: got[i], IDX_AT)
    below = lax.broadcasted_iota(jnp.int32, (8, LANES), 0)
    last = jnp.broadcast_to(coarse_at[...].astype(F32), (8, LANES))
    for t, tile in enumerate(index):
        last = jnp.where(below == t, tile, last)
    for i in range(SIDE):
        for t, tile in enumerate(values + [last]):
            slots[i, :, t * LANES : (t + 1) * LANES] = tile


def coarse_solve(got, high, low, slots, spread, hot, total, rhs):
    width = SIDE * NPRIM
    blocks = high.shape[1] // RADIX
    total[...] = jnp.zeros_like(total)
    rows16 = lax.broadcasted_iota(jnp.int32, (16, LANES), 0).astype(F32)

    def group(step, carry):
        for part in range(2):
            g = step * 2 + part
            tiles = got[g]
            for t in range(width // LANES):
                value = tiles[:, t * LANES : (t + 1) * LANES]
                index = jnp.broadcast_to(tiles[t : t + 1, width : width + LANES], (16, LANES))
                block = jnp.floor(index * (1.0 / RADIX))
                within = (index - block * RADIX).astype(BF16)
                block = block.astype(BF16)
                v_high = value.astype(BF16).astype(F32)
                both = jnp.concatenate([v_high, value - v_high], axis=0).astype(BF16)
                at = part * width + t * LANES
                for l in range(blocks):
                    spread[16 * l : 16 * l + 16, at : at + LANES] = jnp.where(
                        block == jnp.asarray(l, BF16), both, jnp.zeros_like(both)
                    )
                for l in range(RADIX // 16):
                    hot[16 * l : 16 * l + 16, at : at + LANES] = jnp.where(
                        within == (rows16 + 16.0 * l).astype(BF16),
                        jnp.ones_like(both),
                        jnp.zeros_like(both),
                    )
        total[...] += nt(spread[...], hot[...])
        return carry

    lax.fori_loop(0, SIDE // 2, group, 0)
    for l in range(blocks):
        value = total[16 * l : 16 * l + 8] + total[16 * l + 8 : 16 * l + 16]
        v_high = value.astype(BF16).astype(F32)
        rhs[:, l * RADIX : (l + 1) * RADIX] = jnp.concatenate(
            [v_high, value - v_high], axis=0
        ).astype(BF16)
    first = nt(rhs[...], high[...])
    second = nt(rhs[...], low[...])
    solved = first[:8] + first[8:] + second[:8]
    tile = jnp.concatenate([solved, jnp.zeros((8, LANES - NPRIM), F32)], axis=1)
    for i in range(SIDE):
        slots[i] = tile


def pack_solved(place, got, asked, slots):
    width = SIDE * NPRIM
    mine = jnp.concatenate(packed(lambda i: got[i], 0), axis=1)
    parts = jnp.concatenate([p.astype(F32) for p in thirds(mine)], axis=0)
    parts = jnp.concatenate([parts, jnp.zeros((8, width), F32)], axis=0).astype(BF16)
    lane = lax.broadcasted_iota(jnp.int32, (1, LANES), 1)
    for i in range(SIDE):
        want = asked[i, width // LANES : width // LANES + 1, width : width + LANES]
        want = jnp.where(lane < NPRIM, want.astype(jnp.int32) - width * place[0], -1)
        found = nn(parts, one_hot((width, LANES), want))
        slots[i] = found[:8] + found[8:16] + found[16:24]


def corrected(place, got, local_at, local, b, west, south, t_ref, gamma, s0, s1, s2, s3):
    row, col = place[0], place[1]
    rows = got[0]
    for i in range(1, SIDE):
        rows = rows + got[i]
    unknowns = local.shape[1]
    lane = lax.broadcasted_iota(jnp.int32, (8, LANES), 1)
    rows = jnp.where(lane < NPRIM, rows, 0.0)
    correction = selected(rows, one_hot((unknowns, LANES), local_at[...]), nt)
    t = weight_row(row, col, unknowns) * (local[...] + correction)
    t_ref[...] = t
    gamma[...] = jnp.broadcast_to(jnp.sum(b[...] * t, axis=1, keepdims=True), (8, LANES))
    write_sends(t, (west[...], south[...]), row, col, (s0, s1, s2, s3))


def apply_operator(place, t, g0, g1, g2, g3, west, south, high, low, gamma, p_ref, u_ref, s0, s1, s2, s3, slots):
    row, col = place[0], place[1]
    orders = (west[...], south[...])
    p = t[...] + halo([g0[...], g1[...], g2[...], g3[...]], orders, row, col)
    u = times(p, high[...], low[...])
    p_ref[...] = p
    u_ref[...] = u
    write_sends(u, orders, row, col, (s0, s1, s2, s3))
    delta = jnp.broadcast_to(jnp.sum(p * u, axis=1, keepdims=True), (8, LANES))
    lane = lax.broadcasted_iota(jnp.int32, (8, LANES), 1)
    tile = jnp.where(lane == 0, gamma[...], delta)
    for i in range(SIDE):
        slots[i] = tile


def subtotal(got, slots):
    tile = got[0]
    for i in range(1, SIDE):
        tile = tile + got[i]
    for i in range(SIDE):
        slots[i] = tile


def finish(place, got, g0, g1, g2, g3, west, south, p, u, b, solution_ref, residual_ref):
    tile = got[0]
    for i in range(1, SIDE):
        tile = tile + got[i]
    alpha = tile[:, 0:1] / tile[:, 1:2]
    q = u[...] + halo([g0[...], g1[...], g2[...], g3[...]], (west[...], south[...]), place[0], place[1])
    solution_ref[...] = alpha * p[...]
    residual_ref[...] = b[...] - alpha * q


def first_solve(scaled, high, low, local):
    local[...] = times(scaled[...], high[...], low[...])


def sweep(turn):
    def sweep_once(elements, scaled, present, s_high, s_low, f_high, f_low, local):
        rest = scaled[...] - times(present[...], s_high[...], s_low[...])
        after = present[...] + times(rest, f_high[...], f_low[...])
        local[...] = jnp.where(elements[0, 0] // ELEM_BASE > turn, after, present[...])

    return sweep_once


def swapped(sends):
    even = [(i, i ^ 1) for i in range(SIDE)]
    odd = [(i, ((i + 1) ^ 1) - 1) for i in range(1, SIDE - 1)] + [(0, SIDE - 1), (SIDE - 1, 0)]
    return [
        lax.ppermute(x, axis, pairs)
        for x, axis, pairs in zip(sends, (COL, COL, ROW, ROW), (even, odd, even, odd))
    ]


def across(slots, axis):
    return lax.all_to_all(slots, axis, split_axis=0, concat_axis=0, tiled=True)


def body(
    loads, schur, factor, coarse_inverse, elements, west_map, south_map, prim_local, prim_coarse
):
    loads_t = loads[0, 0].T
    unknowns = loads_t.shape[1]
    face = unknowns // 4
    matrix = (unknowns, unknowns)
    place = jnp.stack([lax.axis_index(ROW), lax.axis_index(COL)]).astype(jnp.int32)
    west, south = west_map[0], south_map[0]
    pad = ((0, 0), (0, LANES - NPRIM))
    local_at = jnp.pad(prim_local[0], pad, constant_values=-1)
    coarse_at = jnp.pad(prim_coarse[0], pad)
    field = shape(8, unknowns)
    sends_shape = [shape(8, face)] * 4
    tiles = shape(SIDE, 8, LANES)
    width = SIDE * NPRIM
    product_flops = 2 * 1024 * unknowns * unknowns

    sends = call(first_sends, sends_shape, [SM] + [VM] * 3)(place, loads_t, west, south)
    s_high, s_low, f_high, f_low, c_high, c_low = call(
        split_matrices,
        [shape(*matrix, dtype=BF16)] * 4 + [shape(*coarse_inverse.shape, dtype=BF16)] * 2,
        [VM] * 3,
        flops=product_flops,
    )(schur[0, 0], factor[0, 0], coarse_inverse)
    got = swapped(sends)
    b, scaled, slots = call(right_side, [field, field, tiles], [SM] + [VM] * 9)(
        place, loads_t, *got, west, south, local_at, coarse_at
    )
    local = call(first_solve, field, [VM] * 3, flops=product_flops)(scaled, f_high, f_low)
    for turn in (1, 2):
        local = call(sweep(turn), field, [SM] + [VM] * 6, flops=2 * product_flops)(
            elements, scaled, local, s_high, s_low, f_high, f_low
        )
    gathered = across(slots, COL)
    slots = call(pack_picked, shape(SIDE, 8, width + LANES), [VM] * 2)(gathered, coarse_at)
    asked = across(slots, ROW)
    rows = 16 * coarse_inverse.shape[1] // RADIX
    slots = call(
        coarse_solve,
        tiles,
        [VM] * 3,
        scratch=(
            pltpu.VMEM((rows, 2 * width), BF16),
            pltpu.VMEM((RADIX, 2 * width), BF16),
            pltpu.VMEM((rows, RADIX), F32),
            pltpu.VMEM((16, coarse_inverse.shape[1]), BF16),
        ),
    )(asked, c_high, c_low)
    gathered = across(slots, COL)
    slots = call(pack_solved, tiles, [SM] + [VM] * 2)(place, gathered, asked)
    gathered = across(slots, ROW)
    t, gamma, *sends = call(corrected, [field, shape(8, LANES)] + sends_shape, [SM] + [VM] * 6)(
        place, gathered, local_at, local, b, west, south
    )
    got = swapped(sends)
    p, u, *rest = call(
        apply_operator, [field, field] + sends_shape + [tiles], [SM] + [VM] * 10
    )(place, t, *got, west, south, s_high, s_low, gamma)
    sends, slots = rest[:4], rest[4]
    got = swapped(sends)
    gathered = across(slots, COL)
    slots = call(subtotal, tiles, [VM])(gathered)
    gathered = across(slots, ROW)
    solution, residual = call(finish, [field, field], [SM] + [VM] * 10)(
        place, gathered, *got, west, south, p, u, b
    )
    return solution.T[None, None], residual.T[None, None]


def solution(mesh):
    return jax.shard_map(
        body,
        mesh=mesh,
        in_specs=(
            P(ROW, COL, None, None),
            P(ROW, COL, None, None),
            P(ROW, COL, None, None),
            P((ROW, COL), None),
            P(ROW, COL),
            P(ROW, COL, None),
            P(ROW, COL, None),
            P(ROW, COL, None),
            P(ROW, COL, None),
        ),
        out_specs=(P(ROW, COL, None, None), P(ROW, COL, None, None)),
        check_vma=False,
    )
```

```python
import jax
import jax.numpy as jnp
from jax import lax
from jax.experimental import pallas as pl
from jax.experimental.pallas import tpu as pltpu
from jax.sharding import PartitionSpec as P

ELEM_BASE = 4096
ROW, COL = "row", "col"
F32, BF16 = jnp.float32, jnp.bfloat16
VM = pl.BlockSpec(memory_space=pltpu.VMEM)
SM = pl.BlockSpec(memory_space=pltpu.SMEM)
HB = pl.BlockSpec(memory_space=pltpu.HBM)
CHUNK = 256
LANES = 128
NPRIM = 48
SIDE = 16
IDX_AT = 64
RADIX = 256


def call(body, outs, kinds, scratch=(), flops=0, room=8, grid=(), blocks={}):
    places = {"s": SM, "v": VM, "h": VM, "b": HB}
    kernel = pl.pallas_call(
        body,
        out_shape=outs,
        grid=grid,
        in_specs=[blocks.get(i, places[kind]) for i, kind in enumerate(kinds)],
        out_specs=jax.tree.map(lambda _: VM, outs),
        scratch_shapes=list(scratch),
        cost_estimate=pl.CostEstimate(flops=flops, transcendentals=0, bytes_accessed=0),
        compiler_params=pltpu.CompilerParams(vmem_limit_bytes=room << 20),
        name=body.__name__,
    )

    def run(*args):
        return kernel(
            *(
                x
                if kind == "s"
                else pltpu.with_memory_space_constraint(x, pltpu.VMEM if kind == "v" else pltpu.HBM)
                for x, kind in zip(args, kinds, strict=True)
            )
        )

    return run


def shape(*dims, dtype=F32):
    return pltpu.VMEM(dims, dtype)


def widened(row):
    return jnp.concatenate([row, jnp.zeros((1, LANES - row.shape[1]), row.dtype)], axis=1)


def coordinates():
    return lax.axis_index(ROW), lax.axis_index(COL)


def halves(x):
    high = x.astype(BF16)
    return high, (x - high.astype(F32)).astype(BF16)


def thirds(x):
    high = x.astype(BF16)
    rest = x - high.astype(F32)
    middle = rest.astype(BF16)
    low = (rest - middle.astype(F32)).astype(BF16)
    return high, middle, low


def nn(a, b):
    return lax.dot_general(a, b, (((1,), (0,)), ((), ())), preferred_element_type=F32)


def nt(a, b):
    return lax.dot_general(a, b, (((1,), (1,)), ((), ())), preferred_element_type=F32)


def one_hot(shape_, row):
    return jnp.where(lax.broadcasted_iota(jnp.int32, shape_, 0) == row, 1.0, 0.0).astype(BF16)


def selected(x, matrix, product):
    high, middle, low = thirds(x)
    return product(high, matrix) + product(middle, matrix) + product(low, matrix)


def times(x, high, low):
    x_high, x_low = halves(x)
    return nn(x_high, high) + nn(x_low, high) + nn(x_high, low)


def weight_row(row, col, unknowns):
    face = lax.broadcasted_iota(jnp.int32, (8, unknowns), 1) // (unknowns // 4)
    inner = jnp.where(face == 0, jnp.where(col > 0, 1, 0), jnp.where(col < SIDE - 1, 1, 0))
    outer = jnp.where(face == 2, jnp.where(row > 0, 1, 0), jnp.where(row < SIDE - 1, 1, 0))
    return jnp.where(jnp.where(face < 2, inner, outer) > 0, 0.5, 1.0).astype(F32)


def faces(x):
    size = x.shape[1] // 4
    return [x[:, i * size : (i + 1) * size] for i in range(4)]


def write_sends(values, orders, row, col, sends):
    west, east, south, north = faces(values)
    size = west.shape[1]
    for near, far, order, place, first, second in (
        (west, east, orders[0], col, sends[0], sends[1]),
        (south, north, orders[1], row, sends[2], sends[3]),
    ):
        back = selected(near, one_hot((size, size), order), nt)
        even = place % 2 == 0
        first[...] = jnp.where(even, far, back)
        second[...] = jnp.where(even, back, far)


def halo(got, orders, row, col):
    parts = []
    for order, place, first, second in (
        (orders[0], col, got[0], got[1]),
        (orders[1], row, got[2], got[3]),
    ):
        even = place % 2 == 0
        behind = jnp.where(even, second, first)
        ahead = jnp.where(even, first, second)
        size = behind.shape[1]
        picked = selected(behind, one_hot((size, size), order), nn)
        parts.append(jnp.where(place > 0, picked, 0.0))
        parts.append(jnp.where(place < SIDE - 1, ahead, 0.0))
    return jnp.concatenate(parts, axis=1)


def split_matrix(matrix, high_ref, low_ref):
    high_ref[...], low_ref[...] = halves(matrix[...])


def first_sends(loads, west, south, local_at, coarse_at, s0, s1, s2, s3, *kept):
    row, col = coordinates()
    for ref, value in zip(kept, (loads, west, south, local_at, coarse_at)):
        ref[...] = value[...]
    write_sends(loads[...], (west[...], south[...]), row, col, (s0, s1, s2, s3))


def right_side(loads, g0, g1, g2, g3, west, south, local_at, coarse_at, b_ref, scaled_ref, slots):
    row, col = coordinates()
    b = loads[...] + halo([g0[...], g1[...], g2[...], g3[...]], (west[...], south[...]), row, col)
    scaled = weight_row(row, col, b.shape[1]) * b
    b_ref[...] = b
    scaled_ref[...] = scaled
    picked = selected(scaled, one_hot((b.shape[1], NPRIM), local_at[...]), nn)
    lane = lax.broadcasted_iota(jnp.int32, (8, LANES), 1)
    tile = jnp.concatenate([picked, jnp.zeros((8, LANES - NPRIM), F32)], axis=1)
    index = jnp.broadcast_to(widened(coarse_at[...]).astype(F32), (8, LANES))
    index = pltpu.roll(index, IDX_AT, 1)
    tile = jnp.where((lane >= IDX_AT) & (lane < IDX_AT + NPRIM), index, tile)
    for i in range(SIDE):
        slots[i] = tile


def packed(tile_of, at):
    lane = lax.broadcasted_iota(jnp.int32, (8, LANES), 1)
    count = SIDE * NPRIM // LANES
    out = [jnp.zeros((8, LANES), F32) for _ in range(count)]
    for i in range(SIDE):
        start = i * NPRIM
        t, off = start // LANES, start % LANES
        moved = pltpu.roll(tile_of(i), (off - at) % LANES, 1)
        out[t] = jnp.where((lane >= off) & (lane < off + NPRIM), moved, out[t])
        if off + NPRIM > LANES:
            out[t + 1] = jnp.where(lane < off + NPRIM - LANES, moved, out[t + 1])
    return out


def pack_picked(got, coarse_at, slots):
    values = packed(lambda i: got[i], 0)
    index = packed(lambda i: got[i], IDX_AT)
    below = lax.broadcasted_iota(jnp.int32, (8, LANES), 0)
    last = jnp.broadcast_to(widened(coarse_at[...]).astype(F32), (8, LANES))
    for t, tile in enumerate(index):
        last = jnp.where(below == t, tile, last)
    for i in range(SIDE):
        for t, tile in enumerate(values + [last]):
            slots[i, :, t * LANES : (t + 1) * LANES] = tile


def coarse_solve(got, coarse, slots, spread, hot, total, rhs, here, arrived):
    width = SIDE * NPRIM
    blocks = coarse.shape[1] // RADIX
    copy = pltpu.make_async_copy(coarse, here, arrived)
    copy.start()
    total[...] = jnp.zeros_like(total)
    rows16 = lax.broadcasted_iota(jnp.int32, (16, LANES), 0).astype(F32)

    def group(step, carry):
        for part in range(2):
            g = step * 2 + part
            tiles = got[g]
            for t in range(width // LANES):
                value = tiles[:, t * LANES : (t + 1) * LANES]
                index = jnp.broadcast_to(tiles[t : t + 1, width : width + LANES], (16, LANES))
                block = jnp.floor(index * (1.0 / RADIX))
                within = (index - block * RADIX).astype(BF16)
                block = block.astype(BF16)
                v_high = value.astype(BF16).astype(F32)
                both = jnp.concatenate([v_high, value - v_high], axis=0).astype(BF16)
                at = part * width + t * LANES
                for l in range(blocks):
                    spread[16 * l : 16 * l + 16, at : at + LANES] = jnp.where(
                        block == jnp.asarray(l, BF16), both, jnp.zeros_like(both)
                    )
                for l in range(RADIX // 16):
                    hot[16 * l : 16 * l + 16, at : at + LANES] = jnp.where(
                        within == (rows16 + 16.0 * l).astype(BF16),
                        jnp.ones_like(both),
                        jnp.zeros_like(both),
                    )
        total[...] += nt(spread[...], hot[...])
        return carry

    lax.fori_loop(0, SIDE // 2, group, 0)
    for l in range(blocks):
        value = total[16 * l : 16 * l + 8] + total[16 * l + 8 : 16 * l + 16]
        v_high = value.astype(BF16).astype(F32)
        rhs[:, l * RADIX : (l + 1) * RADIX] = jnp.concatenate(
            [v_high, value - v_high], axis=0
        ).astype(BF16)
    copy.wait()
    high, low = halves(here[...])
    first = nt(rhs[...], high)
    second = nt(rhs[...], low)
    solved = first[:8] + first[8:] + second[:8]
    tile = jnp.concatenate([solved, jnp.zeros((8, LANES - NPRIM), F32)], axis=1)
    for i in range(SIDE):
        slots[i] = tile


def pack_solved(got, asked, slots):
    row, _ = coordinates()
    width = SIDE * NPRIM
    mine = jnp.concatenate(packed(lambda i: got[i], 0), axis=1)
    parts = jnp.concatenate([p.astype(F32) for p in thirds(mine)], axis=0)
    parts = jnp.concatenate([parts, jnp.zeros((8, width), F32)], axis=0).astype(BF16)
    lane = lax.broadcasted_iota(jnp.int32, (1, LANES), 1)
    for i in range(SIDE):
        want = asked[i, width // LANES : width // LANES + 1, width : width + LANES]
        want = jnp.where(lane < NPRIM, want.astype(jnp.int32) - width * row, -1)
        found = nn(parts, one_hot((width, LANES), want))
        slots[i] = found[:8] + found[8:16] + found[16:24]


def corrected(got, local_at, local, b, west, south, t_ref, gamma, s0, s1, s2, s3):
    row, col = coordinates()
    rows = got[0]
    for i in range(1, SIDE):
        rows = rows + got[i]
    unknowns = local.shape[1]
    correction = selected(rows[:, :NPRIM], one_hot((unknowns, NPRIM), local_at[...]), nt)
    t = weight_row(row, col, unknowns) * (local[...] + correction)
    t_ref[...] = t
    gamma[...] = jnp.broadcast_to(jnp.sum(b[...] * t, axis=1, keepdims=True), (8, LANES))
    write_sends(t, (west[...], south[...]), row, col, (s0, s1, s2, s3))


def apply_operator(t, g0, g1, g2, g3, west, south, high, low, gamma, p_ref, u_ref, s0, s1, s2, s3, slots, here, arrived):
    copy = pltpu.make_async_copy(low, here, arrived)
    copy.start()
    row, col = coordinates()
    orders = (west[...], south[...])
    p = t[...] + halo([g0[...], g1[...], g2[...], g3[...]], orders, row, col)
    p_high, p_low = halves(p)
    u = nn(p_high, high[...]) + nn(p_low, high[...])
    copy.wait()
    u = u + nn(p_high, here[...])
    p_ref[...] = p
    u_ref[...] = u
    write_sends(u, orders, row, col, (s0, s1, s2, s3))
    delta = jnp.broadcast_to(jnp.sum(p * u, axis=1, keepdims=True), (8, LANES))
    lane = lax.broadcasted_iota(jnp.int32, (8, LANES), 1)
    tile = jnp.where(lane == 0, gamma[...], delta)
    for i in range(SIDE):
        slots[i] = tile


def subtotal(got, slots):
    tile = got[0]
    for i in range(1, SIDE):
        tile = tile + got[i]
    for i in range(SIDE):
        slots[i] = tile


def finish(got, g0, g1, g2, g3, west, south, p, u, b, solution_ref, residual_ref):
    tile = got[0]
    for i in range(1, SIDE):
        tile = tile + got[i]
    row, col = coordinates()
    alpha = tile[:, 0:1] / tile[:, 1:2]
    q = u[...] + halo([g0[...], g1[...], g2[...], g3[...]], (west[...], south[...]), row, col)
    solution_ref[...] = alpha * p[...]
    residual_ref[...] = b[...] - alpha * q


def chunk_of(ref, k):
    return ref[:, pl.ds(pl.multiple_of(k * CHUNK, CHUNK), CHUNK)]


def first_solve(scaled, factor, local):
    k = pl.program_id(0)
    part = times(chunk_of(scaled, k), *halves(factor[...]))
    local[...] = jnp.where(k == 0, part, local[...] + part)


def sweep(turn):
    def sweep_once(elements, scaled, present, schur, factor, local, rest):
        k = pl.program_id(0)
        half = pl.num_programs(0) // 2

        @pl.when(k < half)
        def _():
            part = times(chunk_of(present, k), *halves(schur[...]))
            rest[...] = jnp.where(k == 0, scaled[...], rest[...]) - part

        @pl.when(k >= half)
        def _():
            part = times(chunk_of(rest, k - half), *halves(factor[...]))
            local[...] = jnp.where(k == half, present[...], local[...]) + part

        @pl.when(k == 2 * half - 1)
        def _():
            done = elements[0, 0] // ELEM_BASE <= turn
            local[...] = jnp.where(done, present[...], local[...])

    return sweep_once


def swapped(sends):
    even = [(i, i ^ 1) for i in range(SIDE)]
    odd = [(i, ((i + 1) ^ 1) - 1) for i in range(1, SIDE - 1)] + [(0, SIDE - 1), (SIDE - 1, 0)]
    return [
        lax.ppermute(x, axis, pairs)
        for x, axis, pairs in zip(sends, (COL, COL, ROW, ROW), (even, odd, even, odd))
    ]


def across(slots, axis):
    return lax.all_to_all(slots, axis, split_axis=0, concat_axis=0, tiled=True)


def body(
    loads, schur, factor, coarse_inverse, elements, west_map, south_map, prim_local, prim_coarse
):
    loads_t = loads[0, 0].T
    unknowns = loads_t.shape[1]
    face = unknowns // 4
    west, south = west_map[0], south_map[0]
    local_at, coarse_at = prim_local[0], prim_coarse[0]
    field = shape(8, unknowns)
    matrix = shape(unknowns, unknowns, dtype=BF16)
    sends_shape = [shape(8, face)] * 4
    tiles = shape(SIDE, 8, LANES)
    width = SIDE * NPRIM
    product_flops = 2 * 1024 * unknowns * unknowns

    kept_shape = [
        pltpu.VMEM(x.shape, x.dtype) for x in (loads_t, west, south, local_at, coarse_at)
    ]
    *sends, loads_t, west, south, local_at, coarse_at = call(
        first_sends, sends_shape + kept_shape, "h" * 5
    )(loads_t, west, south, local_at, coarse_at)
    got = swapped(sends)
    b, scaled, slots = call(right_side, [field, field, tiles], "v" * 9)(
        loads_t, *got, west, south, local_at, coarse_at
    )
    steps = unknowns // CHUNK
    strip = (CHUNK, unknowns)
    matrices = (schur[0, 0], factor[0, 0])
    local = call(
        first_solve,
        field,
        "vh",
        flops=product_flops,
        grid=(steps,),
        blocks={1: pl.BlockSpec(strip, lambda k: (k, 0))},
    )(scaled, matrices[1])
    gathered = across(slots, COL)
    gathered, local = lax.optimization_barrier((gathered, local))
    slots = call(pack_picked, shape(SIDE, 8, width + LANES), "vv")(gathered, coarse_at)

    def swept(turn, local):
        return call(
            sweep(turn),
            field,
            "svvhh",
            scratch=(pltpu.VMEM((8, unknowns), F32),),
            flops=2 * product_flops,
            grid=(2 * steps,),
            blocks={
                3: pl.BlockSpec(strip, lambda k: (jnp.minimum(k, steps - 1), 0)),
                4: pl.BlockSpec(strip, lambda k: (jnp.maximum(k - steps, 0), 0)),
            },
        )(elements, scaled, local, *matrices)

    local = swept(1, local)
    asked = across(slots, ROW)
    asked, local = lax.optimization_barrier((asked, local))
    hot_rows = 16 * coarse_inverse.shape[1] // RADIX
    slots = call(
        coarse_solve,
        tiles,
        "vb",
        room=20,
        scratch=(
            pltpu.VMEM((hot_rows, 2 * width), BF16),
            pltpu.VMEM((RADIX, 2 * width), BF16),
            pltpu.VMEM((hot_rows, RADIX), F32),
            pltpu.VMEM((16, coarse_inverse.shape[1]), BF16),
            pltpu.VMEM(coarse_inverse.shape, F32),
            pltpu.SemaphoreType.DMA,
        ),
    )(asked, coarse_inverse)
    gathered = across(slots, COL)
    local = swept(2, local)
    gathered, local = lax.optimization_barrier((gathered, local))
    slots = call(pack_solved, tiles, "vv")(gathered, asked)
    gathered = across(slots, ROW)
    source, _ = lax.optimization_barrier((matrices[0], local))
    high, low = call(
        split_matrix,
        [matrix, jax.ShapeDtypeStruct((unknowns, unknowns), BF16)],
        "h",
        flops=product_flops,
        room=12,
    )(source)
    gathered, high, low = lax.optimization_barrier((gathered, high, low))
    t, gamma, *sends = call(corrected, [field, shape(8, LANES)] + sends_shape, "v" * 6)(
        gathered, local_at, local, b, west, south
    )
    got = swapped(sends)
    p, u, *rest = call(apply_operator, [field, field] + sends_shape + [tiles], "v" * 8 + "bv", room=12,
        scratch=(pltpu.VMEM((unknowns, unknowns), BF16), pltpu.SemaphoreType.DMA),
    )(t, *got, west, south, high, low, gamma)
    sends, slots = rest[:4], rest[4]
    got = swapped(sends)
    gathered = across(slots, COL)
    gathered, got[0], got[1] = lax.optimization_barrier((gathered, got[0], got[1]))
    slots = call(subtotal, tiles, "v")(gathered)
    gathered = across(slots, ROW)
    whole = jax.ShapeDtypeStruct((8, unknowns), F32)
    solution, residual = call(finish, [whole, whole], "v" * 10)(
        gathered, *got, west, south, p, u, b
    )
    return solution.T[None, None], residual.T[None, None]


def solution(mesh):
    return jax.shard_map(
        body,
        mesh=mesh,
        in_specs=(
            P(ROW, COL, None, None),
            P(ROW, COL, None, None),
            P(ROW, COL, None, None),
            P((ROW, COL), None),
            P(ROW, COL),
            P(ROW, COL, None),
            P(ROW, COL, None),
            P(ROW, COL, None),
            P(ROW, COL, None),
        ),
        out_specs=(P(ROW, COL, None, None), P(ROW, COL, None, None)),
        check_vma=False,
    )
```

```python
import jax
import jax.numpy as jnp
from jax import lax
from jax.experimental import pallas as pl
from jax.experimental.pallas import tpu as pltpu
from jax.sharding import PartitionSpec as P

ELEM_BASE = 4096
ROW, COL = "row", "col"
F32, BF16 = jnp.float32, jnp.bfloat16
VM = pl.BlockSpec(memory_space=pltpu.VMEM)
SM = pl.BlockSpec(memory_space=pltpu.SMEM)
HB = pl.BlockSpec(memory_space=pltpu.HBM)
CHUNK = 256
LANES = 128
NPRIM = 48
SIDE = 16
IDX_AT = 64
RADIX = 256


def call(body, outs, kinds, scratch=(), flops=0, room=8):
    places = {"s": SM, "v": VM, "h": VM, "b": HB}
    kernel = pl.pallas_call(
        body,
        out_shape=outs,
        in_specs=[places[kind] for kind in kinds],
        out_specs=jax.tree.map(lambda _: VM, outs),
        scratch_shapes=list(scratch),
        cost_estimate=pl.CostEstimate(flops=flops, transcendentals=0, bytes_accessed=0),
        compiler_params=pltpu.CompilerParams(vmem_limit_bytes=room << 20),
        name=body.__name__,
    )

    def run(*args):
        return kernel(
            *(
                x
                if kind == "s"
                else pltpu.with_memory_space_constraint(x, pltpu.VMEM if kind == "v" else pltpu.HBM)
                for x, kind in zip(args, kinds, strict=True)
            )
        )

    return run


def shape(*dims, dtype=F32):
    return pltpu.VMEM(dims, dtype)


def widened(row):
    return jnp.concatenate([row, jnp.zeros((1, LANES - row.shape[1]), row.dtype)], axis=1)


def coordinates():
    return lax.axis_index(ROW), lax.axis_index(COL)


def halves(x):
    high = x.astype(BF16)
    return high, (x - high.astype(F32)).astype(BF16)


def thirds(x):
    high = x.astype(BF16)
    rest = x - high.astype(F32)
    middle = rest.astype(BF16)
    low = (rest - middle.astype(F32)).astype(BF16)
    return high, middle, low


def nn(a, b):
    return lax.dot_general(a, b, (((1,), (0,)), ((), ())), preferred_element_type=F32)


def nt(a, b):
    return lax.dot_general(a, b, (((1,), (1,)), ((), ())), preferred_element_type=F32)


def one_hot(shape_, row):
    return jnp.where(lax.broadcasted_iota(jnp.int32, shape_, 0) == row, 1.0, 0.0).astype(BF16)


def selected(x, matrix, product):
    high, middle, low = thirds(x)
    return product(high, matrix) + product(middle, matrix) + product(low, matrix)


def times(x, high, low):
    x_high, x_low = halves(x)
    return nn(x_high, high) + nn(x_low, high) + nn(x_high, low)


def weight_row(row, col, unknowns):
    face = lax.broadcasted_iota(jnp.int32, (8, unknowns), 1) // (unknowns // 4)
    inner = jnp.where(face == 0, jnp.where(col > 0, 1, 0), jnp.where(col < SIDE - 1, 1, 0))
    outer = jnp.where(face == 2, jnp.where(row > 0, 1, 0), jnp.where(row < SIDE - 1, 1, 0))
    return jnp.where(jnp.where(face < 2, inner, outer) > 0, 0.5, 1.0).astype(F32)


def faces(x):
    size = x.shape[1] // 4
    return [x[:, i * size : (i + 1) * size] for i in range(4)]


def write_sends(values, orders, row, col, sends):
    west, east, south, north = faces(values)
    size = west.shape[1]
    for near, far, order, place, first, second in (
        (west, east, orders[0], col, sends[0], sends[1]),
        (south, north, orders[1], row, sends[2], sends[3]),
    ):
        back = selected(near, one_hot((size, size), order), nt)
        even = place % 2 == 0
        first[...] = jnp.where(even, far, back)
        second[...] = jnp.where(even, back, far)


def halo(got, orders, row, col):
    parts = []
    for order, place, first, second in (
        (orders[0], col, got[0], got[1]),
        (orders[1], row, got[2], got[3]),
    ):
        even = place % 2 == 0
        behind = jnp.where(even, second, first)
        ahead = jnp.where(even, first, second)
        size = behind.shape[1]
        picked = selected(behind, one_hot((size, size), order), nn)
        parts.append(jnp.where(place > 0, picked, 0.0))
        parts.append(jnp.where(place < SIDE - 1, ahead, 0.0))
    return jnp.concatenate(parts, axis=1)


def split_matrix(matrix, high_ref, low_ref):
    high_ref[...], low_ref[...] = halves(matrix[...])


def first_sends(loads, west, south, local_at, coarse_at, s0, s1, s2, s3, *kept):
    row, col = coordinates()
    for ref, value in zip(kept, (loads, west, south, local_at, coarse_at)):
        ref[...] = value[...]
    write_sends(loads[...], (west[...], south[...]), row, col, (s0, s1, s2, s3))


def right_side(loads, g0, g1, g2, g3, west, south, local_at, coarse_at, b_ref, scaled_ref, slots):
    row, col = coordinates()
    b = loads[...] + halo([g0[...], g1[...], g2[...], g3[...]], (west[...], south[...]), row, col)
    scaled = weight_row(row, col, b.shape[1]) * b
    b_ref[...] = b
    scaled_ref[...] = scaled
    picked = selected(scaled, one_hot((b.shape[1], NPRIM), local_at[...]), nn)
    lane = lax.broadcasted_iota(jnp.int32, (8, LANES), 1)
    tile = jnp.concatenate([picked, jnp.zeros((8, LANES - NPRIM), F32)], axis=1)
    index = jnp.broadcast_to(widened(coarse_at[...]).astype(F32), (8, LANES))
    index = pltpu.roll(index, IDX_AT, 1)
    tile = jnp.where((lane >= IDX_AT) & (lane < IDX_AT + NPRIM), index, tile)
    for i in range(SIDE):
        slots[i] = tile


def packed(tile_of, at):
    lane = lax.broadcasted_iota(jnp.int32, (8, LANES), 1)
    count = SIDE * NPRIM // LANES
    out = [jnp.zeros((8, LANES), F32) for _ in range(count)]
    for i in range(SIDE):
        start = i * NPRIM
        t, off = start // LANES, start % LANES
        moved = pltpu.roll(tile_of(i), (off - at) % LANES, 1)
        out[t] = jnp.where((lane >= off) & (lane < off + NPRIM), moved, out[t])
        if off + NPRIM > LANES:
            out[t + 1] = jnp.where(lane < off + NPRIM - LANES, moved, out[t + 1])
    return out


def pack_picked(got, coarse_at, slots):
    values = packed(lambda i: got[i], 0)
    index = packed(lambda i: got[i], IDX_AT)
    below = lax.broadcasted_iota(jnp.int32, (8, LANES), 0)
    last = jnp.broadcast_to(widened(coarse_at[...]).astype(F32), (8, LANES))
    for t, tile in enumerate(index):
        last = jnp.where(below == t, tile, last)
    for i in range(SIDE):
        for t, tile in enumerate(values + [last]):
            slots[i, :, t * LANES : (t + 1) * LANES] = tile


def coarse_solve(got, coarse, slots, spread, hot, total, rhs, here, arrived):
    width = SIDE * NPRIM
    blocks = coarse.shape[1] // RADIX
    copy = pltpu.make_async_copy(coarse, here, arrived)
    copy.start()
    total[...] = jnp.zeros_like(total)
    rows16 = lax.broadcasted_iota(jnp.int32, (16, LANES), 0).astype(F32)

    def group(step, carry):
        for part in range(2):
            g = step * 2 + part
            tiles = got[g]
            for t in range(width // LANES):
                value = tiles[:, t * LANES : (t + 1) * LANES]
                index = jnp.broadcast_to(tiles[t : t + 1, width : width + LANES], (16, LANES))
                block = jnp.floor(index * (1.0 / RADIX))
                within = (index - block * RADIX).astype(BF16)
                block = block.astype(BF16)
                v_high = value.astype(BF16).astype(F32)
                both = jnp.concatenate([v_high, value - v_high], axis=0).astype(BF16)
                at = part * width + t * LANES
                for l in range(blocks):
                    spread[16 * l : 16 * l + 16, at : at + LANES] = jnp.where(
                        block == jnp.asarray(l, BF16), both, jnp.zeros_like(both)
                    )
                for l in range(RADIX // 16):
                    hot[16 * l : 16 * l + 16, at : at + LANES] = jnp.where(
                        within == (rows16 + 16.0 * l).astype(BF16),
                        jnp.ones_like(both),
                        jnp.zeros_like(both),
                    )
        total[...] += nt(spread[...], hot[...])
        return carry

    lax.fori_loop(0, SIDE // 2, group, 0)
    for l in range(blocks):
        value = total[16 * l : 16 * l + 8] + total[16 * l + 8 : 16 * l + 16]
        v_high = value.astype(BF16).astype(F32)
        rhs[:, l * RADIX : (l + 1) * RADIX] = jnp.concatenate(
            [v_high, value - v_high], axis=0
        ).astype(BF16)
    copy.wait()
    high, low = halves(here[...])
    first = nt(rhs[...], high)
    second = nt(rhs[...], low)
    solved = first[:8] + first[8:] + second[:8]
    tile = jnp.concatenate([solved, jnp.zeros((8, LANES - NPRIM), F32)], axis=1)
    for i in range(SIDE):
        slots[i] = tile


def pack_solved(got, asked, slots):
    row, _ = coordinates()
    width = SIDE * NPRIM
    mine = jnp.concatenate(packed(lambda i: got[i], 0), axis=1)
    parts = jnp.concatenate([p.astype(F32) for p in thirds(mine)], axis=0)
    parts = jnp.concatenate([parts, jnp.zeros((8, width), F32)], axis=0).astype(BF16)
    lane = lax.broadcasted_iota(jnp.int32, (1, LANES), 1)
    for i in range(SIDE):
        want = asked[i, width // LANES : width // LANES + 1, width : width + LANES]
        want = jnp.where(lane < NPRIM, want.astype(jnp.int32) - width * row, -1)
        found = nn(parts, one_hot((width, LANES), want))
        slots[i] = found[:8] + found[8:16] + found[16:24]


def corrected(got, local_at, local, b, west, south, t_ref, gamma, s0, s1, s2, s3):
    row, col = coordinates()
    rows = got[0]
    for i in range(1, SIDE):
        rows = rows + got[i]
    unknowns = local.shape[1]
    correction = selected(rows[:, :NPRIM], one_hot((unknowns, NPRIM), local_at[...]), nt)
    t = weight_row(row, col, unknowns) * (local[...] + correction)
    t_ref[...] = t
    gamma[...] = jnp.broadcast_to(jnp.sum(b[...] * t, axis=1, keepdims=True), (8, LANES))
    write_sends(t, (west[...], south[...]), row, col, (s0, s1, s2, s3))


def apply_operator(t, g0, g1, g2, g3, west, south, high, low, gamma, p_ref, u_ref, s0, s1, s2, s3, slots, here, arrived):
    copy = pltpu.make_async_copy(low, here, arrived)
    copy.start()
    row, col = coordinates()
    orders = (west[...], south[...])
    p = t[...] + halo([g0[...], g1[...], g2[...], g3[...]], orders, row, col)
    p_high, p_low = halves(p)
    u = nn(p_high, high[...]) + nn(p_low, high[...])
    copy.wait()
    u = u + nn(p_high, here[...])
    p_ref[...] = p
    u_ref[...] = u
    write_sends(u, orders, row, col, (s0, s1, s2, s3))
    delta = jnp.broadcast_to(jnp.sum(p * u, axis=1, keepdims=True), (8, LANES))
    lane = lax.broadcasted_iota(jnp.int32, (8, LANES), 1)
    tile = jnp.where(lane == 0, gamma[...], delta)
    for i in range(SIDE):
        slots[i] = tile


def subtotal(got, slots):
    tile = got[0]
    for i in range(1, SIDE):
        tile = tile + got[i]
    for i in range(SIDE):
        slots[i] = tile


def finish(got, g0, g1, g2, g3, west, south, p, u, b, solution_ref, residual_ref):
    tile = got[0]
    for i in range(1, SIDE):
        tile = tile + got[i]
    row, col = coordinates()
    alpha = tile[:, 0:1] / tile[:, 1:2]
    q = u[...] + halo([g0[...], g1[...], g2[...], g3[...]], (west[...], south[...]), row, col)
    solution_ref[...] = alpha * p[...]
    residual_ref[...] = b[...] - alpha * q


def strips(matrices, here, arrived):
    count = matrices[0].shape[0] // CHUNK
    copies = []
    for i, matrix in enumerate(matrices):
        for k in range(count):
            at = i * count + k
            copies.append(
                pltpu.make_async_copy(
                    matrix.at[pl.ds(k * CHUNK, CHUNK)], here.at[at], arrived.at[at]
                )
            )
    for copy in copies:
        copy.start()

    def product(i, x):
        total = None
        for k in range(count):
            at = i * count + k
            copies[at].wait()
            part = times(x[:, k * CHUNK : (k + 1) * CHUNK], *halves(here[at]))
            total = part if total is None else total + part
        return total

    return product


def first_solve(scaled, factor, local, here, arrived):
    local[...] = strips((factor,), here, arrived)(0, scaled[...])


def sweep(turn):
    def sweep_once(elements, scaled, present, schur, factor, local, here, arrived):
        product = strips((schur, factor), here, arrived)
        before = present[...]
        after = before + product(1, scaled[...] - product(0, before))
        local[...] = jnp.where(elements[0, 0] // ELEM_BASE > turn, after, before)

    return sweep_once


def swapped(sends):
    even = [(i, i ^ 1) for i in range(SIDE)]
    odd = [(i, ((i + 1) ^ 1) - 1) for i in range(1, SIDE - 1)]
    return [
        lax.ppermute(x, axis, pairs)
        for x, axis, pairs in zip(sends, (COL, COL, ROW, ROW), (even, odd, even, odd))
    ]


def across(slots, axis):
    return lax.all_to_all(slots, axis, split_axis=0, concat_axis=0, tiled=True)


def body(
    loads, schur, factor, coarse_inverse, elements, west_map, south_map, prim_local, prim_coarse
):
    loads_t = loads[0, 0].T
    unknowns = loads_t.shape[1]
    face = unknowns // 4
    west, south = west_map[0], south_map[0]
    local_at, coarse_at = prim_local[0], prim_coarse[0]
    field = shape(8, unknowns)
    matrix = shape(unknowns, unknowns, dtype=BF16)
    sends_shape = [shape(8, face)] * 4
    tiles = shape(SIDE, 8, LANES)
    width = SIDE * NPRIM
    product_flops = 2 * 1024 * unknowns * unknowns

    kept_shape = [
        pltpu.VMEM(x.shape, x.dtype) for x in (loads_t, west, south, local_at, coarse_at)
    ]
    *sends, loads_t, west, south, local_at, coarse_at = call(
        first_sends, sends_shape + kept_shape, "h" * 5
    )(loads_t, west, south, local_at, coarse_at)
    got = swapped(sends)
    b, scaled, slots = call(right_side, [field, field, tiles], "v" * 9)(
        loads_t, *got, west, south, local_at, coarse_at
    )
    steps = unknowns // CHUNK

    def landing(count):
        return pltpu.VMEM((count, CHUNK, unknowns), F32), pltpu.SemaphoreType.DMA((count,))

    matrices = (schur[0, 0], factor[0, 0])
    local = call(
        first_solve,
        field,
        "vb",
        flops=product_flops,
        room=12,
        scratch=landing(steps),
    )(scaled, matrices[1])
    gathered = across(slots, COL)
    gathered, local = lax.optimization_barrier((gathered, local))
    slots = call(pack_picked, shape(SIDE, 8, width + LANES), "vv")(gathered, coarse_at)

    def swept(turn, local):
        return call(
            sweep(turn),
            field,
            "svvbb",
            scratch=landing(2 * steps),
            flops=2 * product_flops,
            room=18,
        )(elements, scaled, local, *matrices)

    local = swept(1, local)
    asked = across(slots, ROW)
    asked, local = lax.optimization_barrier((asked, local))
    hot_rows = 16 * coarse_inverse.shape[1] // RADIX
    slots = call(
        coarse_solve,
        tiles,
        "vb",
        room=20,
        scratch=(
            pltpu.VMEM((hot_rows, 2 * width), BF16),
            pltpu.VMEM((RADIX, 2 * width), BF16),
            pltpu.VMEM((hot_rows, RADIX), F32),
            pltpu.VMEM((16, coarse_inverse.shape[1]), BF16),
            pltpu.VMEM(coarse_inverse.shape, F32),
            pltpu.SemaphoreType.DMA,
        ),
    )(asked, coarse_inverse)
    gathered = across(slots, COL)
    local = swept(2, local)
    gathered, local = lax.optimization_barrier((gathered, local))
    slots = call(pack_solved, tiles, "vv")(gathered, asked)
    gathered = across(slots, ROW)
    source, _ = lax.optimization_barrier((matrices[0], local))
    high, low = call(
        split_matrix,
        [matrix, jax.ShapeDtypeStruct((unknowns, unknowns), BF16)],
        "h",
        flops=product_flops,
        room=12,
    )(source)
    gathered, high, low = lax.optimization_barrier((gathered, high, low))
    t, gamma, *sends = call(corrected, [field, shape(8, LANES)] + sends_shape, "v" * 6)(
        gathered, local_at, local, b, west, south
    )
    got = swapped(sends)
    p, u, *rest = call(apply_operator, [field, field] + sends_shape + [tiles], "v" * 8 + "bv", room=12,
        scratch=(pltpu.VMEM((unknowns, unknowns), BF16), pltpu.SemaphoreType.DMA),
    )(t, *got, west, south, high, low, gamma)
    sends, slots = rest[:4], rest[4]
    got = swapped(sends)
    gathered = across(slots, COL)
    gathered, got[0], got[1] = lax.optimization_barrier((gathered, got[0], got[1]))
    slots = call(subtotal, tiles, "v")(gathered)
    gathered = across(slots, ROW)
    whole = jax.ShapeDtypeStruct((8, unknowns), F32)
    solution, residual = call(finish, [whole, whole], "v" * 10)(
        gathered, *got, west, south, p, u, b
    )
    return solution.T[None, None], residual.T[None, None]


def solution(mesh):
    return jax.shard_map(
        body,
        mesh=mesh,
        in_specs=(
            P(ROW, COL, None, None),
            P(ROW, COL, None, None),
            P(ROW, COL, None, None),
            P((ROW, COL), None),
            P(ROW, COL),
            P(ROW, COL, None),
            P(ROW, COL, None),
            P(ROW, COL, None),
            P(ROW, COL, None),
        ),
        out_specs=(P(ROW, COL, None, None), P(ROW, COL, None, None)),
        check_vma=False,
    )
```

```python
import jax
import jax.numpy as jnp
from jax import lax
from jax.experimental import pallas as pl
from jax.experimental.pallas import tpu as pltpu
from jax.sharding import PartitionSpec as P

ELEM_BASE = 4096
ROW, COL = "row", "col"
F32, BF16 = jnp.float32, jnp.bfloat16
VM = pl.BlockSpec(memory_space=pltpu.VMEM)
SM = pl.BlockSpec(memory_space=pltpu.SMEM)
HB = pl.BlockSpec(memory_space=pltpu.HBM)
CHUNK = 256
LANES = 128
NPRIM = 48
SIDE = 16
IDX_AT = 64
RADIX = 256


def call(body, outs, kinds, scratch=(), flops=0, room=8):
    places = {"s": SM, "v": VM, "h": VM, "b": HB}
    kernel = pl.pallas_call(
        body,
        out_shape=outs,
        in_specs=[places[kind] for kind in kinds],
        out_specs=jax.tree.map(lambda _: VM, outs),
        scratch_shapes=list(scratch),
        cost_estimate=pl.CostEstimate(flops=flops, transcendentals=0, bytes_accessed=0),
        compiler_params=pltpu.CompilerParams(vmem_limit_bytes=room << 20),
        name=body.__name__,
    )

    def run(*args):
        return kernel(
            *(
                x
                if kind == "s"
                else pltpu.with_memory_space_constraint(x, pltpu.VMEM if kind == "v" else pltpu.HBM)
                for x, kind in zip(args, kinds, strict=True)
            )
        )

    return run


def shape(*dims, dtype=F32):
    return pltpu.VMEM(dims, dtype)


def widened(row):
    return jnp.concatenate([row, jnp.zeros((1, LANES - row.shape[1]), row.dtype)], axis=1)


def coordinates():
    return lax.axis_index(ROW), lax.axis_index(COL)


def halves(x):
    high = x.astype(BF16)
    return high, (x - high.astype(F32)).astype(BF16)


def thirds(x):
    high = x.astype(BF16)
    rest = x - high.astype(F32)
    middle = rest.astype(BF16)
    low = (rest - middle.astype(F32)).astype(BF16)
    return high, middle, low


def nn(a, b):
    return lax.dot_general(a, b, (((1,), (0,)), ((), ())), preferred_element_type=F32)


def nt(a, b):
    return lax.dot_general(a, b, (((1,), (1,)), ((), ())), preferred_element_type=F32)


def one_hot(shape_, row):
    return jnp.where(lax.broadcasted_iota(jnp.int32, shape_, 0) == row, 1.0, 0.0).astype(BF16)


def selected(x, matrix, product):
    high, middle, low = thirds(x)
    return product(high, matrix) + product(middle, matrix) + product(low, matrix)


def times(x, high, low):
    x_high, x_low = halves(x)
    return nn(x_high, high) + nn(x_low, high) + nn(x_high, low)


def weight_row(row, col, unknowns):
    face = lax.broadcasted_iota(jnp.int32, (8, unknowns), 1) // (unknowns // 4)
    inner = jnp.where(face == 0, jnp.where(col > 0, 1, 0), jnp.where(col < SIDE - 1, 1, 0))
    outer = jnp.where(face == 2, jnp.where(row > 0, 1, 0), jnp.where(row < SIDE - 1, 1, 0))
    return jnp.where(jnp.where(face < 2, inner, outer) > 0, 0.5, 1.0).astype(F32)


def faces(x):
    size = x.shape[1] // 4
    return [x[:, i * size : (i + 1) * size] for i in range(4)]


def write_sends(values, orders, row, col, sends):
    west, east, south, north = faces(values)
    size = west.shape[1]
    for near, far, order, place, first, second in (
        (west, east, orders[0], col, sends[0], sends[1]),
        (south, north, orders[1], row, sends[2], sends[3]),
    ):
        back = selected(near, one_hot((size, size), order), nt)
        even = place % 2 == 0
        first[...] = jnp.where(even, far, back)
        second[...] = jnp.where(even, back, far)


def halo(got, orders, row, col):
    parts = []
    for order, place, first, second in (
        (orders[0], col, got[0], got[1]),
        (orders[1], row, got[2], got[3]),
    ):
        even = place % 2 == 0
        behind = jnp.where(even, second, first)
        ahead = jnp.where(even, first, second)
        size = behind.shape[1]
        picked = selected(behind, one_hot((size, size), order), nn)
        parts.append(jnp.where(place > 0, picked, 0.0))
        parts.append(jnp.where(place < SIDE - 1, ahead, 0.0))
    return jnp.concatenate(parts, axis=1)


def split_matrix(matrix, high_ref, low_ref):
    high_ref[...], low_ref[...] = halves(matrix[...])


def first_sends(loads, west, south, local_at, coarse_at, s0, s1, s2, s3, *kept):
    row, col = coordinates()
    for ref, value in zip(kept, (loads, west, south, local_at, coarse_at)):
        ref[...] = value[...]
    write_sends(loads[...], (west[...], south[...]), row, col, (s0, s1, s2, s3))


def right_side(loads, g0, g1, g2, g3, west, south, local_at, coarse_at, b_ref, scaled_ref, slots):
    row, col = coordinates()
    b = loads[...] + halo([g0[...], g1[...], g2[...], g3[...]], (west[...], south[...]), row, col)
    scaled = weight_row(row, col, b.shape[1]) * b
    b_ref[...] = b
    scaled_ref[...] = scaled
    picked = selected(scaled, one_hot((b.shape[1], NPRIM), local_at[...]), nn)
    lane = lax.broadcasted_iota(jnp.int32, (8, LANES), 1)
    tile = jnp.concatenate([picked, jnp.zeros((8, LANES - NPRIM), F32)], axis=1)
    index = jnp.broadcast_to(widened(coarse_at[...]).astype(F32), (8, LANES))
    index = pltpu.roll(index, IDX_AT, 1)
    tile = jnp.where((lane >= IDX_AT) & (lane < IDX_AT + NPRIM), index, tile)
    for i in range(SIDE):
        slots[i] = tile


def packed(tile_of, at):
    lane = lax.broadcasted_iota(jnp.int32, (8, LANES), 1)
    count = SIDE * NPRIM // LANES
    out = [jnp.zeros((8, LANES), F32) for _ in range(count)]
    for i in range(SIDE):
        start = i * NPRIM
        t, off = start // LANES, start % LANES
        moved = pltpu.roll(tile_of(i), (off - at) % LANES, 1)
        out[t] = jnp.where((lane >= off) & (lane < off + NPRIM), moved, out[t])
        if off + NPRIM > LANES:
            out[t + 1] = jnp.where(lane < off + NPRIM - LANES, moved, out[t + 1])
    return out


def pack_picked(got, coarse_at, slots):
    values = packed(lambda i: got[i], 0)
    index = packed(lambda i: got[i], IDX_AT)
    below = lax.broadcasted_iota(jnp.int32, (8, LANES), 0)
    last = jnp.broadcast_to(widened(coarse_at[...]).astype(F32), (8, LANES))
    for t, tile in enumerate(index):
        last = jnp.where(below == t, tile, last)
    for i in range(SIDE):
        for t, tile in enumerate(values + [last]):
            slots[i, :, t * LANES : (t + 1) * LANES] = tile


def coarse_solve(got, coarse, slots, spread, hot, total, rhs, here, arrived):
    width = SIDE * NPRIM
    blocks = coarse.shape[1] // RADIX
    copy = pltpu.make_async_copy(coarse, here, arrived)
    copy.start()
    total[...] = jnp.zeros_like(total)
    rows16 = lax.broadcasted_iota(jnp.int32, (16, LANES), 0).astype(F32)

    def group(step, carry):
        for part in range(2):
            g = step * 2 + part
            tiles = got[g]
            for t in range(width // LANES):
                value = tiles[:, t * LANES : (t + 1) * LANES]
                index = jnp.broadcast_to(tiles[t : t + 1, width : width + LANES], (16, LANES))
                block = jnp.floor(index * (1.0 / RADIX))
                within = (index - block * RADIX).astype(BF16)
                block = block.astype(BF16)
                v_high = value.astype(BF16).astype(F32)
                both = jnp.concatenate([v_high, value - v_high], axis=0).astype(BF16)
                at = part * width + t * LANES
                for l in range(blocks):
                    spread[16 * l : 16 * l + 16, at : at + LANES] = jnp.where(
                        block == jnp.asarray(l, BF16), both, jnp.zeros_like(both)
                    )
                for l in range(RADIX // 16):
                    hot[16 * l : 16 * l + 16, at : at + LANES] = jnp.where(
                        within == (rows16 + 16.0 * l).astype(BF16),
                        jnp.ones_like(both),
                        jnp.zeros_like(both),
                    )
        total[...] += nt(spread[...], hot[...])
        return carry

    lax.fori_loop(0, SIDE // 2, group, 0)
    for l in range(blocks):
        value = total[16 * l : 16 * l + 8] + total[16 * l + 8 : 16 * l + 16]
        v_high = value.astype(BF16).astype(F32)
        rhs[:, l * RADIX : (l + 1) * RADIX] = jnp.concatenate(
            [v_high, value - v_high], axis=0
        ).astype(BF16)
    copy.wait()
    high, low = halves(here[...])
    first = nt(rhs[...], high)
    second = nt(rhs[...], low)
    solved = first[:8] + first[8:] + second[:8]
    tile = jnp.concatenate([solved, jnp.zeros((8, LANES - NPRIM), F32)], axis=1)
    for i in range(SIDE):
        slots[i] = tile


def pack_solved(got, asked, slots):
    row, _ = coordinates()
    width = SIDE * NPRIM
    mine = jnp.concatenate(packed(lambda i: got[i], 0), axis=1)
    parts = jnp.concatenate([p.astype(F32) for p in thirds(mine)], axis=0)
    parts = jnp.concatenate([parts, jnp.zeros((8, width), F32)], axis=0).astype(BF16)
    lane = lax.broadcasted_iota(jnp.int32, (1, LANES), 1)
    for i in range(SIDE):
        want = asked[i, width // LANES : width // LANES + 1, width : width + LANES]
        want = jnp.where(lane < NPRIM, want.astype(jnp.int32) - width * row, -1)
        found = nn(parts, one_hot((width, LANES), want))
        slots[i] = found[:8] + found[8:16] + found[16:24]


def corrected(got, local_at, local, b, west, south, t_ref, gamma, s0, s1, s2, s3):
    row, col = coordinates()
    rows = got[0]
    for i in range(1, SIDE):
        rows = rows + got[i]
    unknowns = local.shape[1]
    correction = selected(rows[:, :NPRIM], one_hot((unknowns, NPRIM), local_at[...]), nt)
    t = weight_row(row, col, unknowns) * (local[...] + correction)
    t_ref[...] = t
    gamma[...] = jnp.broadcast_to(jnp.sum(b[...] * t, axis=1, keepdims=True), (8, LANES))
    write_sends(t, (west[...], south[...]), row, col, (s0, s1, s2, s3))


def apply_operator(t, g0, g1, g2, g3, west, south, high, low, gamma, p_ref, u_ref, s0, s1, s2, s3, slots, here, arrived):
    copy = pltpu.make_async_copy(low, here, arrived)
    copy.start()
    row, col = coordinates()
    orders = (west[...], south[...])
    p = t[...] + halo([g0[...], g1[...], g2[...], g3[...]], orders, row, col)
    p_high, p_low = halves(p)
    u = nn(p_high, high[...]) + nn(p_low, high[...])
    copy.wait()
    u = u + nn(p_high, here[...])
    p_ref[...] = p
    u_ref[...] = u
    write_sends(u, orders, row, col, (s0, s1, s2, s3))
    delta = jnp.broadcast_to(jnp.sum(p * u, axis=1, keepdims=True), (8, LANES))
    lane = lax.broadcasted_iota(jnp.int32, (8, LANES), 1)
    tile = jnp.where(lane == 0, gamma[...], delta)
    for i in range(SIDE):
        slots[i] = tile


def subtotal(got, slots):
    tile = got[0]
    for i in range(1, SIDE):
        tile = tile + got[i]
    for i in range(SIDE):
        slots[i] = tile


def finish(got, g0, g1, g2, g3, west, south, p, u, b, solution_ref, residual_ref):
    tile = got[0]
    for i in range(1, SIDE):
        tile = tile + got[i]
    row, col = coordinates()
    alpha = tile[:, 0:1] / tile[:, 1:2]
    q = u[...] + halo([g0[...], g1[...], g2[...], g3[...]], (west[...], south[...]), row, col)
    solution_ref[...] = alpha * p[...]
    residual_ref[...] = b[...] - alpha * q


def strips(matrices, here, arrived):
    count = matrices[0].shape[0] // CHUNK
    copies = []
    for i, matrix in enumerate(matrices):
        for k in range(count):
            at = i * count + k
            copies.append(
                pltpu.make_async_copy(
                    matrix.at[pl.ds(k * CHUNK, CHUNK)], here.at[at], arrived.at[at]
                )
            )
    for copy in copies:
        copy.start()

    def product(i, x):
        total = None
        for k in range(count):
            at = i * count + k
            copies[at].wait()
            part = times(x[:, k * CHUNK : (k + 1) * CHUNK], *halves(here[at]))
            total = part if total is None else total + part
        return total

    return product


def first_solve(scaled, factor, local, here, arrived):
    local[...] = strips((factor,), here, arrived)(0, scaled[...])


def sweep(turn):
    def sweep_once(elements, scaled, present, schur, factor, local, here, arrived):
        product = strips((schur, factor), here, arrived)
        before = present[...]
        after = before + product(1, scaled[...] - product(0, before))
        local[...] = jnp.where(elements[0, 0] // ELEM_BASE > turn, after, before)

    return sweep_once


def swapped(sends):
    even = [(i, i ^ 1) for i in range(SIDE)]
    odd = [(i, ((i + 1) ^ 1) - 1) for i in range(1, SIDE - 1)] + [(0, SIDE - 1), (SIDE - 1, 0)]
    return [
        lax.ppermute(x, axis, pairs)
        for x, axis, pairs in zip(sends, (COL, COL, ROW, ROW), (even, odd, even, odd))
    ]


def across(slots, axis):
    return lax.all_to_all(slots, axis, split_axis=0, concat_axis=0, tiled=True)


def body(
    loads, schur, factor, coarse_inverse, elements, west_map, south_map, prim_local, prim_coarse
):
    loads_t = loads[0, 0].T
    unknowns = loads_t.shape[1]
    face = unknowns // 4
    west, south = west_map[0], south_map[0]
    local_at, coarse_at = prim_local[0], prim_coarse[0]
    field = shape(8, unknowns)
    matrix = shape(unknowns, unknowns, dtype=BF16)
    sends_shape = [shape(8, face)] * 4
    tiles = shape(SIDE, 8, LANES)
    width = SIDE * NPRIM
    product_flops = 2 * 1024 * unknowns * unknowns

    kept_shape = [
        pltpu.VMEM(x.shape, x.dtype) for x in (loads_t, west, south, local_at, coarse_at)
    ]
    *sends, loads_t, west, south, local_at, coarse_at = call(
        first_sends, sends_shape + kept_shape, "h" * 5
    )(loads_t, west, south, local_at, coarse_at)
    got = swapped(sends)
    b, scaled, slots = call(right_side, [field, field, tiles], "v" * 9)(
        loads_t, *got, west, south, local_at, coarse_at
    )
    steps = unknowns // CHUNK

    def landing(count):
        return pltpu.VMEM((count, CHUNK, unknowns), F32), pltpu.SemaphoreType.DMA((count,))

    matrices = (schur[0, 0], factor[0, 0])
    local = call(
        first_solve,
        field,
        "vb",
        flops=product_flops,
        room=12,
        scratch=landing(steps),
    )(scaled, matrices[1])
    gathered = across(slots, COL)
    gathered, local = lax.optimization_barrier((gathered, local))
    slots = call(pack_picked, shape(SIDE, 8, width + LANES), "vv")(gathered, coarse_at)

    def swept(turn, local):
        return call(
            sweep(turn),
            field,
            "svvbb",
            scratch=landing(2 * steps),
            flops=2 * product_flops,
            room=18,
        )(elements, scaled, local, *matrices)

    local = swept(1, local)
    asked = across(slots, ROW)
    asked, local = lax.optimization_barrier((asked, local))
    hot_rows = 16 * coarse_inverse.shape[1] // RADIX
    slots = call(
        coarse_solve,
        tiles,
        "vb",
        room=20,
        scratch=(
            pltpu.VMEM((hot_rows, 2 * width), BF16),
            pltpu.VMEM((RADIX, 2 * width), BF16),
            pltpu.VMEM((hot_rows, RADIX), F32),
            pltpu.VMEM((16, coarse_inverse.shape[1]), BF16),
            pltpu.VMEM(coarse_inverse.shape, F32),
            pltpu.SemaphoreType.DMA,
        ),
    )(asked, coarse_inverse)
    gathered = across(slots, COL)
    local = swept(2, local)
    gathered, local = lax.optimization_barrier((gathered, local))
    slots = call(pack_solved, tiles, "vv")(gathered, asked)
    gathered = across(slots, ROW)
    source, _ = lax.optimization_barrier((matrices[0], local))
    high, low = call(
        split_matrix,
        [matrix, jax.ShapeDtypeStruct((unknowns, unknowns), BF16)],
        "h",
        flops=product_flops,
        room=12,
    )(source)
    gathered, high, low = lax.optimization_barrier((gathered, high, low))
    t, gamma, *sends = call(corrected, [field, shape(8, LANES)] + sends_shape, "v" * 6)(
        gathered, local_at, local, b, west, south
    )
    got = swapped(sends)
    p, u, *rest = call(apply_operator, [field, field] + sends_shape + [tiles], "v" * 8 + "bv", room=12,
        scratch=(pltpu.VMEM((unknowns, unknowns), BF16), pltpu.SemaphoreType.DMA),
    )(t, *got, west, south, high, low, gamma)
    sends, slots = rest[:4], rest[4]
    got = swapped(sends)
    gathered = across(slots, COL)
    gathered, got[0], got[1] = lax.optimization_barrier((gathered, got[0], got[1]))
    slots = call(subtotal, tiles, "v")(gathered)
    gathered = across(slots, ROW)
    whole = jax.ShapeDtypeStruct((8, unknowns), F32)
    solution, residual = call(finish, [whole, whole], "v" * 10)(
        gathered, *got, west, south, p, u, b
    )
    return solution.T[None, None], residual.T[None, None]


def solution(mesh):
    return jax.shard_map(
        body,
        mesh=mesh,
        in_specs=(
            P(ROW, COL, None, None),
            P(ROW, COL, None, None),
            P(ROW, COL, None, None),
            P((ROW, COL), None),
            P(ROW, COL),
            P(ROW, COL, None),
            P(ROW, COL, None),
            P(ROW, COL, None),
            P(ROW, COL, None),
        ),
        out_specs=(P(ROW, COL, None, None), P(ROW, COL, None, None)),
        check_vma=False,
    )
```

```python
import jax
import jax.numpy as jnp
from jax import lax
from jax.experimental import pallas as pl
from jax.experimental.pallas import tpu as pltpu
from jax.sharding import PartitionSpec as P

ELEM_BASE = 4096
ROW, COL = "row", "col"
F32, BF16 = jnp.float32, jnp.bfloat16
VM = pl.BlockSpec(memory_space=pltpu.VMEM)
SM = pl.BlockSpec(memory_space=pltpu.SMEM)
HB = pl.BlockSpec(memory_space=pltpu.HBM)
CHUNK = 256
LANES = 128
NPRIM = 48
SIDE = 16
IDX_AT = 64
RADIX = 256


def call(body, outs, kinds, scratch=(), flops=0, room=8):
    places = {"s": SM, "v": VM, "h": VM, "b": HB}
    kernel = pl.pallas_call(
        body,
        out_shape=outs,
        in_specs=[places[kind] for kind in kinds],
        out_specs=jax.tree.map(lambda _: VM, outs),
        scratch_shapes=list(scratch),
        cost_estimate=pl.CostEstimate(flops=flops, transcendentals=0, bytes_accessed=0),
        compiler_params=pltpu.CompilerParams(vmem_limit_bytes=room << 20),
        name=body.__name__,
    )

    def run(*args):
        return kernel(
            *(
                x
                if kind == "s"
                else pltpu.with_memory_space_constraint(x, pltpu.VMEM if kind == "v" else pltpu.HBM)
                for x, kind in zip(args, kinds, strict=True)
            )
        )

    return run


def shape(*dims, dtype=F32):
    return pltpu.VMEM(dims, dtype)


def widened(row):
    return jnp.concatenate([row, jnp.zeros((1, LANES - row.shape[1]), row.dtype)], axis=1)


def coordinates():
    return lax.axis_index(ROW), lax.axis_index(COL)


def halves(x):
    high = x.astype(BF16)
    return high, (x - high.astype(F32)).astype(BF16)


def thirds(x):
    high = x.astype(BF16)
    rest = x - high.astype(F32)
    middle = rest.astype(BF16)
    low = (rest - middle.astype(F32)).astype(BF16)
    return high, middle, low


def nn(a, b):
    return lax.dot_general(a, b, (((1,), (0,)), ((), ())), preferred_element_type=F32)


def nt(a, b):
    return lax.dot_general(a, b, (((1,), (1,)), ((), ())), preferred_element_type=F32)


def one_hot(shape_, row):
    return jnp.where(lax.broadcasted_iota(jnp.int32, shape_, 0) == row, 1.0, 0.0).astype(BF16)


def selected(x, matrix, product):
    high, middle, low = thirds(x)
    return product(high, matrix) + product(middle, matrix) + product(low, matrix)


def times(x, high, low):
    x_high, x_low = halves(x)
    return nn(x_high, high) + nn(x_low, high) + nn(x_high, low)


def weight_row(row, col, unknowns):
    face = lax.broadcasted_iota(jnp.int32, (8, unknowns), 1) // (unknowns // 4)
    inner = jnp.where(face == 0, jnp.where(col > 0, 1, 0), jnp.where(col < SIDE - 1, 1, 0))
    outer = jnp.where(face == 2, jnp.where(row > 0, 1, 0), jnp.where(row < SIDE - 1, 1, 0))
    return jnp.where(jnp.where(face < 2, inner, outer) > 0, 0.5, 1.0).astype(F32)


def faces(x):
    size = x.shape[1] // 4
    return [x[:, i * size : (i + 1) * size] for i in range(4)]


def write_sends(values, orders, row, col, sends):
    west, east, south, north = faces(values)
    size = west.shape[1]
    for near, far, order, place, first, second in (
        (west, east, orders[0], col, sends[0], sends[1]),
        (south, north, orders[1], row, sends[2], sends[3]),
    ):
        back = selected(near, one_hot((size, size), order), nt)
        even = place % 2 == 0
        first[...] = jnp.where(even, far, back)
        second[...] = jnp.where(even, back, far)


def halo(got, orders, row, col):
    parts = []
    for order, place, first, second in (
        (orders[0], col, got[0], got[1]),
        (orders[1], row, got[2], got[3]),
    ):
        even = place % 2 == 0
        behind = jnp.where(even, second, first)
        ahead = jnp.where(even, first, second)
        size = behind.shape[1]
        picked = selected(behind, one_hot((size, size), order), nn)
        parts.append(jnp.where(place > 0, picked, 0.0))
        parts.append(jnp.where(place < SIDE - 1, ahead, 0.0))
    return jnp.concatenate(parts, axis=1)


def split_matrix(matrix, high_ref, low_ref):
    high_ref[...], low_ref[...] = halves(matrix[...])


def first_sends(loads, west, south, local_at, coarse_at, s0, s1, s2, s3, *kept):
    row, col = coordinates()
    for ref, value in zip(kept, (loads, west, south, local_at, coarse_at)):
        ref[...] = value[...]
    write_sends(loads[...], (west[...], south[...]), row, col, (s0, s1, s2, s3))


def right_side(loads, g0, g1, g2, g3, west, south, local_at, coarse_at, b_ref, scaled_ref, slots):
    row, col = coordinates()
    b = loads[...] + halo([g0[...], g1[...], g2[...], g3[...]], (west[...], south[...]), row, col)
    scaled = weight_row(row, col, b.shape[1]) * b
    b_ref[...] = b
    scaled_ref[...] = scaled
    picked = selected(scaled, one_hot((b.shape[1], NPRIM), local_at[...]), nn)
    lane = lax.broadcasted_iota(jnp.int32, (8, LANES), 1)
    tile = jnp.concatenate([picked, jnp.zeros((8, LANES - NPRIM), F32)], axis=1)
    index = jnp.broadcast_to(widened(coarse_at[...]).astype(F32), (8, LANES))
    index = pltpu.roll(index, IDX_AT, 1)
    tile = jnp.where((lane >= IDX_AT) & (lane < IDX_AT + NPRIM), index, tile)
    for i in range(SIDE):
        slots[i] = tile


def packed(tile_of, at):
    lane = lax.broadcasted_iota(jnp.int32, (8, LANES), 1)
    count = SIDE * NPRIM // LANES
    out = [jnp.zeros((8, LANES), F32) for _ in range(count)]
    for i in range(SIDE):
        start = i * NPRIM
        t, off = start // LANES, start % LANES
        moved = pltpu.roll(tile_of(i), (off - at) % LANES, 1)
        out[t] = jnp.where((lane >= off) & (lane < off + NPRIM), moved, out[t])
        if off + NPRIM > LANES:
            out[t + 1] = jnp.where(lane < off + NPRIM - LANES, moved, out[t + 1])
    return out


def pack_picked(got, coarse_at, slots):
    values = packed(lambda i: got[i], 0)
    index = packed(lambda i: got[i], IDX_AT)
    below = lax.broadcasted_iota(jnp.int32, (8, LANES), 0)
    last = jnp.broadcast_to(widened(coarse_at[...]).astype(F32), (8, LANES))
    for t, tile in enumerate(index):
        last = jnp.where(below == t, tile, last)
    for i in range(SIDE):
        for t, tile in enumerate(values + [last]):
            slots[i, :, t * LANES : (t + 1) * LANES] = tile


def coarse_solve(got, coarse, slots, spread, hot, total, rhs, here, arrived):
    width = SIDE * NPRIM
    blocks = coarse.shape[1] // RADIX
    copy = pltpu.make_async_copy(coarse, here, arrived)
    copy.start()
    total[...] = jnp.zeros_like(total)
    rows16 = lax.broadcasted_iota(jnp.int32, (16, LANES), 0).astype(F32)

    def group(step, carry):
        for part in range(2):
            g = step * 2 + part
            tiles = got[g]
            for t in range(width // LANES):
                value = tiles[:, t * LANES : (t + 1) * LANES]
                index = jnp.broadcast_to(tiles[t : t + 1, width : width + LANES], (16, LANES))
                block = jnp.floor(index * (1.0 / RADIX))
                within = (index - block * RADIX).astype(BF16)
                block = block.astype(BF16)
                v_high = value.astype(BF16).astype(F32)
                both = jnp.concatenate([v_high, value - v_high], axis=0).astype(BF16)
                at = part * width + t * LANES
                for l in range(blocks):
                    spread[16 * l : 16 * l + 16, at : at + LANES] = jnp.where(
                        block == jnp.asarray(l, BF16), both, jnp.zeros_like(both)
                    )
                for l in range(RADIX // 16):
                    hot[16 * l : 16 * l + 16, at : at + LANES] = jnp.where(
                        within == (rows16 + 16.0 * l).astype(BF16),
                        jnp.ones_like(both),
                        jnp.zeros_like(both),
                    )
        total[...] += nt(spread[...], hot[...])
        return carry

    lax.fori_loop(0, SIDE // 2, group, 0)
    for l in range(blocks):
        value = total[16 * l : 16 * l + 8] + total[16 * l + 8 : 16 * l + 16]
        v_high = value.astype(BF16).astype(F32)
        rhs[:, l * RADIX : (l + 1) * RADIX] = jnp.concatenate(
            [v_high, value - v_high], axis=0
        ).astype(BF16)
    copy.wait()
    high, low = halves(here[...])
    first = nt(rhs[...], high)
    second = nt(rhs[...], low)
    solved = first[:8] + first[8:] + second[:8]
    tile = jnp.concatenate([solved, jnp.zeros((8, LANES - NPRIM), F32)], axis=1)
    for i in range(SIDE):
        slots[i] = tile


def pack_solved(got, asked, slots):
    row, _ = coordinates()
    width = SIDE * NPRIM
    mine = jnp.concatenate(packed(lambda i: got[i], 0), axis=1)
    parts = jnp.concatenate([p.astype(F32) for p in thirds(mine)], axis=0)
    parts = jnp.concatenate([parts, jnp.zeros((8, width), F32)], axis=0).astype(BF16)
    lane = lax.broadcasted_iota(jnp.int32, (1, LANES), 1)
    for i in range(SIDE):
        want = asked[i, width // LANES : width // LANES + 1, width : width + LANES]
        want = jnp.where(lane < NPRIM, want.astype(jnp.int32) - width * row, -1)
        found = nn(parts, one_hot((width, LANES), want))
        slots[i] = found[:8] + found[8:16] + found[16:24]


def corrected(got, local_at, local, b, west, south, t_ref, gamma, s0, s1, s2, s3):
    row, col = coordinates()
    rows = got[0]
    for i in range(1, SIDE):
        rows = rows + got[i]
    unknowns = local.shape[1]
    correction = selected(rows[:, :NPRIM], one_hot((unknowns, NPRIM), local_at[...]), nt)
    t = weight_row(row, col, unknowns) * (local[...] + correction)
    t_ref[...] = t
    gamma[...] = jnp.broadcast_to(jnp.sum(b[...] * t, axis=1, keepdims=True), (8, LANES))
    write_sends(t, (west[...], south[...]), row, col, (s0, s1, s2, s3))


def apply_operator(t, g0, g1, g2, g3, west, south, high, low, gamma, p_ref, u_ref, s0, s1, s2, s3, slots, here, arrived):
    copy = pltpu.make_async_copy(low, here, arrived)
    copy.start()
    row, col = coordinates()
    orders = (west[...], south[...])
    p = t[...] + halo([g0[...], g1[...], g2[...], g3[...]], orders, row, col)
    p_high, p_low = halves(p)
    u = nn(p_high, high[...]) + nn(p_low, high[...])
    copy.wait()
    u = u + nn(p_high, here[...])
    p_ref[...] = p
    u_ref[...] = u
    write_sends(u, orders, row, col, (s0, s1, s2, s3))
    delta = jnp.broadcast_to(jnp.sum(p * u, axis=1, keepdims=True), (8, LANES))
    lane = lax.broadcasted_iota(jnp.int32, (8, LANES), 1)
    tile = jnp.where(lane == 0, gamma[...], delta)
    for i in range(SIDE):
        slots[i] = tile


def subtotal(got, slots):
    tile = got[0]
    for i in range(1, SIDE):
        tile = tile + got[i]
    for i in range(SIDE):
        slots[i] = tile


def finish(got, g0, g1, g2, g3, west, south, p, u, b, solution_ref, residual_ref):
    tile = got[0]
    for i in range(1, SIDE):
        tile = tile + got[i]
    row, col = coordinates()
    alpha = tile[:, 0:1] / tile[:, 1:2]
    q = u[...] + halo([g0[...], g1[...], g2[...], g3[...]], (west[...], south[...]), row, col)
    solution_ref[...] = alpha * p[...]
    residual_ref[...] = b[...] - alpha * q


def strips(matrices, here, arrived):
    count = matrices[0].shape[0] // CHUNK
    copies = []
    for i, matrix in enumerate(matrices):
        for k in range(count):
            at = i * count + k
            copies.append(
                pltpu.make_async_copy(
                    matrix.at[pl.ds(k * CHUNK, CHUNK)], here.at[at], arrived.at[at]
                )
            )
    for copy in copies:
        copy.start()

    def product(i, x):
        total = None
        for k in range(count):
            at = i * count + k
            copies[at].wait()
            part = times(x[:, k * CHUNK : (k + 1) * CHUNK], *halves(here[at]))
            total = part if total is None else total + part
        return total

    return product


def first_solve(scaled, factor, local, here, arrived):
    local[...] = strips((factor,), here, arrived)(0, scaled[...])


def sweep(turn):
    def sweep_once(elements, scaled, present, schur, factor, local, here, arrived):
        product = strips((schur, factor), here, arrived)
        before = present[...]
        after = before + product(1, scaled[...] - product(0, before))
        local[...] = jnp.where(elements[0, 0] // ELEM_BASE > turn, after, before)

    return sweep_once


def swapped(sends):
    even = [(i, i ^ 1) for i in range(SIDE)]
    odd = [(i, ((i + 1) ^ 1) - 1) for i in range(1, SIDE - 1)] + [(0, SIDE - 1), (SIDE - 1, 0)]
    return [
        lax.ppermute(x, axis, pairs)
        for x, axis, pairs in zip(sends, (COL, COL, ROW, ROW), (even, odd, even, odd))
    ]


def across(slots, axis):
    return lax.all_to_all(slots, axis, split_axis=0, concat_axis=0, tiled=True)


def body(
    loads, schur, factor, coarse_inverse, elements, west_map, south_map, prim_local, prim_coarse
):
    loads_t = loads[0, 0].T
    unknowns = loads_t.shape[1]
    face = unknowns // 4
    west, south = west_map[0], south_map[0]
    local_at, coarse_at = prim_local[0], prim_coarse[0]
    field = shape(8, unknowns)
    matrix = shape(unknowns, unknowns, dtype=BF16)
    sends_shape = [shape(8, face)] * 4
    tiles = shape(SIDE, 8, LANES)
    width = SIDE * NPRIM
    product_flops = 2 * 1024 * unknowns * unknowns

    kept_shape = [
        pltpu.VMEM(x.shape, x.dtype) for x in (loads_t, west, south, local_at, coarse_at)
    ]
    *sends, loads_t, west, south, local_at, coarse_at = call(
        first_sends, sends_shape + kept_shape, "h" * 5
    )(loads_t, west, south, local_at, coarse_at)
    got = swapped(sends)
    b, scaled, slots = call(right_side, [field, field, tiles], "v" * 9)(
        loads_t, *got, west, south, local_at, coarse_at
    )
    steps = unknowns // CHUNK

    def landing(count):
        return pltpu.VMEM((count, CHUNK, unknowns), F32), pltpu.SemaphoreType.DMA((count,))

    matrices = (schur[0, 0], factor[0, 0])
    local = call(
        first_solve,
        field,
        "vb",
        flops=product_flops,
        room=12,
        scratch=landing(steps),
    )(scaled, matrices[1])
    gathered = across(slots, COL)
    gathered, local = lax.optimization_barrier((gathered, local))
    slots = call(pack_picked, shape(SIDE, 8, width + LANES), "vv")(gathered, coarse_at)

    def swept(turn, local):
        return call(
            sweep(turn),
            field,
            "svvbb",
            scratch=landing(2 * steps),
            flops=2 * product_flops,
            room=18,
        )(elements, scaled, local, *matrices)

    local = swept(1, local)
    asked = across(slots, ROW)
    asked, local = lax.optimization_barrier((asked, local))
    hot_rows = 16 * coarse_inverse.shape[1] // RADIX
    slots = call(
        coarse_solve,
        tiles,
        "vb",
        room=20,
        scratch=(
            pltpu.VMEM((hot_rows, 2 * width), BF16),
            pltpu.VMEM((RADIX, 2 * width), BF16),
            pltpu.VMEM((hot_rows, RADIX), F32),
            pltpu.VMEM((16, coarse_inverse.shape[1]), BF16),
            pltpu.VMEM(coarse_inverse.shape, F32),
            pltpu.SemaphoreType.DMA,
        ),
    )(asked, coarse_inverse)
    gathered = across(slots, COL)
    local = swept(2, local)
    gathered, local = lax.optimization_barrier((gathered, local))
    slots = call(pack_solved, tiles, "vv")(gathered, asked)
    gathered = across(slots, ROW)
    source, _ = lax.optimization_barrier((matrices[0], local))
    high, low = call(
        split_matrix,
        [matrix, jax.ShapeDtypeStruct((unknowns, unknowns), BF16)],
        "h",
        flops=product_flops,
        room=12,
    )(source)
    gathered, high, low = lax.optimization_barrier((gathered, high, low))
    t, gamma, *sends = call(corrected, [field, shape(8, LANES)] + sends_shape, "v" * 6)(
        gathered, local_at, local, b, west, south
    )
    got = swapped(sends)
    p, u, *rest = call(apply_operator, [field, field] + sends_shape + [tiles], "v" * 8 + "bv", room=12,
        scratch=(pltpu.VMEM((unknowns, unknowns), BF16), pltpu.SemaphoreType.DMA),
    )(t, *got, west, south, high, low, gamma)
    sends, slots = rest[:4], rest[4]
    got = swapped(sends)
    gathered = across(slots, COL)
    gathered, got[2], got[3] = lax.optimization_barrier((gathered, got[2], got[3]))
    slots = call(subtotal, tiles, "v")(gathered)
    gathered = across(slots, ROW)
    whole = jax.ShapeDtypeStruct((8, unknowns), F32)
    solution, residual = call(finish, [whole, whole], "v" * 10)(
        gathered, *got, west, south, p, u, b
    )
    return solution.T[None, None], residual.T[None, None]


def solution(mesh):
    return jax.shard_map(
        body,
        mesh=mesh,
        in_specs=(
            P(ROW, COL, None, None),
            P(ROW, COL, None, None),
            P(ROW, COL, None, None),
            P((ROW, COL), None),
            P(ROW, COL),
            P(ROW, COL, None),
            P(ROW, COL, None),
            P(ROW, COL, None),
            P(ROW, COL, None),
        ),
        out_specs=(P(ROW, COL, None, None), P(ROW, COL, None, None)),
        check_vma=False,
    )
```
